256 devices in a mesh: span: 256 (over y, x, z, core).
Axes of the slice: x: 4, y: 4, z: 8, core: 2. Of those that a mesh axis runs over, the one named last changes fastest.
Arguments:
- returns: bfloat16 [256, 2097152], P(None, 'span'), may hold values from -40 to 40
- market: bfloat16 [2097152], P('span'), may hold values from -12 to 12
- mask: int32 [2097152], P('span'), may hold values 0 or 1
- counts: int32 [256], P('span'), may hold values from 0 to 8192, as said below
Outputs:
- slope: float32 [256, 1048576], P(None, 'span')
The draws below stay inside these ranges and needn't reach their ends.
Inputs may be any that keep to these rules, and one draw needn't show every extreme that they name: For every span d, the counts of spans 0 to d sum to between (d + 1) * 4096 and (d + 2) * 4096; all counts sum to exactly 1048576; some span holds exactly 8192.
All inputs are finite; a program needn't handle non-finite values. No bound on the sum of `mask` on one device may be relied on, other than what follows from the above.
Results may differ from the reference program's by a relative error of at most 0.00039.
Values may be sent and summed in bfloat16 or wider, within the bound.
A program may use at most 64 MiB of HBM per device.

```python
import jax
import jax.numpy as jnp
from jax import lax

STOCKS = 256
WIN = 1024
BLOCK = 512
QROWS = 4096
CAP = 8192
N_SPAN = 256


def series_parts(key):
    row_total = N_SPAN * 2 * QROWS
    subkeys = jax.random.split(jax.random.fold_in(key, 11), 4)
    market = jax.random.normal(subkeys[0], (row_total,), jnp.float32)
    noise_part = jax.random.normal(subkeys[1], (STOCKS, row_total), jnp.float32)
    market = jnp.clip(market, -12.0, 12.0)
    beta_load = jax.random.uniform(subkeys[2], (STOCKS, 1), jnp.float32, 0.4, 1.8)
    regime = 1.0 + 0.6 * jax.random.uniform(subkeys[3], (STOCKS, row_total // BLOCK), jnp.float32, -1.0, 1.0)
    regime = jnp.repeat(regime, BLOCK, axis=1)
    returns = jnp.clip(beta_load * regime * market[None, :] + noise_part, -40.0, 40.0)
    return (returns, market)


def draw_returns(key, part):
    return series_parts(key)[0].astype(jnp.bfloat16)


def draw_market(key, part):
    return series_parts(key)[1].astype(jnp.bfloat16)


def draw_counts(key, part):
    excess = jax.random.randint(jax.random.fold_in(key, 3), (N_SPAN,), 0, QROWS + 1)
    excess = excess.at[N_SPAN - 3].set(QROWS)
    chosen = jax.random.randint(jax.random.fold_in(key, 5), (), 1, N_SPAN - 2)
    excess = excess.at[chosen].set(QROWS)
    excess = excess.at[chosen - 1].set(0)
    excess = excess.at[N_SPAN - 1].set(0)
    previous = jnp.concatenate([jnp.zeros((1,), jnp.int32), excess[:-1]])
    return (QROWS + excess - previous).astype(jnp.int32)


def plant(result, stream_key, least, top_value):
    dims = result.shape
    index_at = [jax.random.randint(jax.random.fold_in(stream_key, axis), (), 0, dims[axis]) for axis in range(len(dims))]
    result = result.at[tuple(index_at)].set(least)
    longest = dims.index(max(dims))
    index_at[longest] = (index_at[longest] + 1) % dims[longest]
    return result.at[tuple(index_at)].set(top_value)


def setup_inputs(seed: int = 0) -> dict:
    seeds = jax.random.split(jax.random.key(seed), 5)
    return {
        "returns": draw_returns(jax.random.fold_in(seeds[4], 71), 0),
        "market": draw_market(jax.random.fold_in(seeds[4], 71), 0),
        "mask": plant((jax.random.randint(seeds[2], (N_SPAN * CAP,), 0, 8) < 7).astype(jnp.int32), jax.random.fold_in(seeds[2], 1), 0, 1),
        "counts": draw_counts(jax.random.fold_in(seeds[4], 71), 0),
    }


RIDGE = 0.1


def band_matrix():
    row_index = jnp.arange(BLOCK + WIN, dtype=jnp.int32)[:, None]
    col_index = jnp.arange(BLOCK, dtype=jnp.int32)[None, :]
    inside = (row_index >= col_index + 1) & (row_index <= col_index + WIN)
    return inside.astype(jnp.bfloat16)


def stacked(y_values, x_values, w_values):
    cross_terms = (x_values.astype(jnp.float32)[None, :] * y_values.astype(jnp.float32)).astype(jnp.bfloat16)
    square = (x_values.astype(jnp.float32) * x_values.astype(jnp.float32)).astype(jnp.bfloat16)
    return jnp.concatenate([cross_terms, y_values, w_values[None, :], x_values[None, :], square[None, :]], 0)


def slopes_of(moments):
    stocks = (moments.shape[0] - 3) // 2
    sum_xy = moments[:stocks]
    sum_y = moments[stocks:2 * stocks]
    sum_w = moments[2 * stocks]
    sum_x = moments[2 * stocks + 1]
    sum_xx = moments[2 * stocks + 2]
    numerator = sum_w * sum_xy - sum_x * sum_y
    denominator = sum_w * sum_xx - sum_x * sum_x + RIDGE * WIN * WIN
    return numerator / denominator


def reference(returns, market, mask, counts):
    capacity = 2 * QROWS
    tick_total = QROWS * N_SPAN
    before = (jnp.cumsum(counts) - counts).astype(jnp.int32)
    row_index = jnp.arange(capacity, dtype=jnp.int32)
    destination = before[:, None] + row_index[None, :]
    destination = jnp.where(row_index[None, :] < counts[:, None], destination, tick_total).reshape(-1).astype(jnp.int32)
    weight = mask.astype(jnp.float32)
    y_values = (returns.astype(jnp.float32) * weight[None, :]).astype(jnp.bfloat16)
    x_values = (market.astype(jnp.float32) * weight).astype(jnp.bfloat16)
    y_ticks = jnp.zeros((STOCKS, tick_total), jnp.bfloat16).at[:, destination].set(y_values, mode="drop")
    x_ticks = jnp.zeros((tick_total,), jnp.bfloat16).at[destination].set(x_values, mode="drop")
    w_ticks = jnp.zeros((tick_total,), jnp.bfloat16).at[destination].set(weight.astype(jnp.bfloat16), mode="drop")
    stacked_rows = stacked(y_ticks, x_ticks, w_ticks)
    extended = jnp.concatenate([jnp.zeros((stacked_rows.shape[0], WIN), jnp.bfloat16), stacked_rows], 1)
    band_ones = band_matrix()

    def one_block(block_index):
        window_piece = lax.dynamic_slice_in_dim(extended, block_index * BLOCK, BLOCK + WIN, 1)
        return slopes_of(jnp.dot(window_piece, band_ones, preferred_element_type=jnp.float32))

    blocks = lax.map(one_block, jnp.arange(tick_total // BLOCK, dtype=jnp.int32))
    return jnp.transpose(blocks, (1, 0, 2)).reshape(STOCKS, tick_total)
```

```python
import functools

import jax
import jax.numpy as jnp
from jax import lax
from jax.experimental import pallas as pl
from jax.experimental.pallas import tpu as pltpu
from jax.sharding import PartitionSpec as P

WIN = 1024
QROWS = 4096
CAP = 2 * QROWS
REACH = QROWS + WIN
RIDGE = 0.1
LANES = 128
TILE = 256
RT = REACH // LANES
OT = CAP // LANES
TT = WIN // LANES
MESH = pl.DeviceIdType.MESH
ZS, XS, YS = 8, 4, 4


def rolled(load, start, tiles, rows):
    first = lax.shift_right_logical(start, 7)
    r = jnp.bitwise_and(start, LANES - 1)
    turn = jnp.bitwise_and(LANES - r, LANES - 1)
    keep = lax.broadcasted_iota(jnp.int32, (rows, LANES), 1) < LANES - r
    turned = [pltpu.roll(load(first + j), turn, 1) for j in range(tiles + 1)]
    return [jnp.where(keep, turned[j], turned[j + 1]) for j in range(tiles)]


def clamped(ref, row, rows, index):
    index = jnp.minimum(jnp.maximum(index, 0), ref.shape[1] // LANES - 1)
    return ref[row : row + rows, pl.ds(pl.multiple_of(index * LANES, LANES), LANES)]


def moved_right(tiles, ticks, count):
    r = jnp.bitwise_and(ticks, LANES - 1)
    turned = [pltpu.roll(tile, r, 1) for tile in tiles]
    low = lax.broadcasted_iota(jnp.int32, tiles[0].shape, 1) < r
    n = len(tiles)
    at = {i: jnp.where(low, turned[max(i - 1, 0)], turned[min(i, n - 1)]) for i in range(n + 1)}
    for bit in (32, 16, 8, 4, 2, 1):
        taken = jnp.bitwise_and(ticks, bit * LANES) != 0
        moved = {}
        for i in range(count):
            if i in at and i - bit in at:
                moved[i] = jnp.where(taken, at[i - bit], at[i])
            elif i in at or i - bit in at:
                moved[i] = at[i] if i in at else at[i - bit]
        at = moved
    return at


def exchange_kernel(groups, rows, counts, returns, xw, near, far, nearx, farx, place, *scratch):
    n = groups + 1
    it = iter(scratch)
    take = lambda: [next(it) for _ in range(n)]
    ends, send, tiled = take(), take(), take()
    pairin, zbuf, xbuf, ybuf, ebuf = (next(it) for _ in range(5))
    near_ssem, cross_ssem, near_rsem, far_ssem, far_rsem, cnt_ssem, cnt_rsem = (next(it) for _ in range(7))

    me = lax.axis_index("span")
    total = ZS * XS * YS * 2
    even = lax.rem(me, 2) == 0
    odd = lax.rem(me, 2) == 1
    last = me == total - 1
    chip = lax.div(me, 2)
    z = lax.rem(chip, ZS)
    x = lax.rem(lax.div(chip, ZS), XS)
    y = lax.div(chip, ZS * XS)

    def core0(yy, xx, zz):
        return ((yy * XS + xx) * ZS + zz) * 2

    def at_z(step):
        return core0(y, x, lax.rem(z + step + ZS, ZS))

    def at_x(step):
        return core0(y, lax.rem(x + step, XS), z)

    def at_y(step):
        return core0(lax.rem(y + step, YS), x, z)

    order = [groups] + list(range(groups))

    def remote(src, dst, ssem, rsem, target):
        return pltpu.make_async_remote_copy(
            src_ref=src, dst_ref=dst, send_sem=ssem, recv_sem=rsem, device_id=(target,), device_id_type=MESH
        )

    def source(g):
        return (xw, 0, 2) if g == groups else (returns, g * rows, rows)

    def near_at(g):
        return nearx if g == groups else near.at[pl.ds(g * rows, rows), :]

    def far_at(g):
        return farx if g == groups else far.at[pl.ds(g * rows, rows), :]

    barrier = pltpu.get_barrier_semaphore()

    def hello(target):
        pl.semaphore_signal(barrier, inc=1, device_id=(target,), device_id_type=MESH)

    mine = counts[0]

    @pl.when(me == 0)
    def _():
        near[...] = jnp.zeros_like(near)
        nearx[...] = jnp.zeros_like(nearx)

    @pl.when(even)
    def _():
        hello(me + 1)
        for step in (1, 2, -1, -2):
            hello(at_z(step))
        for step in (1, 2, 3):
            hello(at_x(step))
            hello(at_y(step))

        @pl.when(me > 0)
        def _():
            hello(me - 1)

    @pl.when(odd)
    def _():
        hello(me - 1)

        @pl.when(jnp.logical_not(last))
        def _():
            hello(me + 1)

    def end_window(g):
        ref, row, m = source(g)
        for t in range(OT):
            tiled[g][t] = ref[row : row + m, t * LANES : (t + 1) * LANES]
        slot = lambda k: tiled[g][jnp.minimum(jnp.maximum(k - RT, 0), OT - 1)]
        for j, value in enumerate(rolled(slot, mine, RT, m)):
            ends[g][:, j * LANES : (j + 1) * LANES] = value

    pairin[...] = jnp.zeros_like(pairin) + mine
    end_window(order[0])
    end_window(order[1])

    @pl.when(even)
    def _():
        pl.semaphore_wait(barrier, 11 + jnp.where(me > 0, 1, 0))

    @pl.when(odd)
    def _():
        pl.semaphore_wait(barrier, 2 - jnp.where(last, 1, 0))
        remote(pairin, zbuf.at[0], cnt_ssem.at[0], cnt_rsem.at[0], me - 1).start()

    for i, g in enumerate(order):
        if i > 1:
            end_window(g)

        @pl.when(even)
        def _(g=g):
            remote(ends[g], near_at(g), near_ssem.at[g], near_rsem.at[g], me + 1).start()

    @pl.when(odd)
    def _():
        short = jnp.maximum(REACH - mine, 0)
        for g in order:
            remote(ends[g], near_at(g), near_ssem.at[g], near_rsem.at[g], me - 1).wait_recv()

            @pl.when(jnp.logical_not(last))
            def _(g=g):
                ref, row, m = (nearx, 0, 2) if g == groups else (near, g * rows, rows)
                for first in range(0, m, 16):
                    part = min(m, 16)
                    a = slice(row + first, row + first + part)
                    tail = [ref[a, QROWS + j * LANES : QROWS + (j + 1) * LANES] for j in range(TT)]
                    placed = moved_right(tail, short, RT + TT)
                    lane = lax.broadcasted_iota(jnp.int32, (part, LANES), 1)
                    for j in range(RT):
                        b, c = slice(first, first + part), slice(j * LANES, (j + 1) * LANES)
                        send[g][b, c] = jnp.where(lane < short - j * LANES, placed[j + TT], ends[g][b, c])
                remote(send[g], near_at(g), cross_ssem.at[g], near_rsem.at[g], me + 1).start()

    @pl.when(even)
    def _():
        def arrival(dst, k):
            return remote(dst, dst, cnt_ssem.at[k], cnt_rsem.at[k], me + 1)

        sends = []

        def push(ref, target, k):
            copy = remote(ref, ref, cnt_ssem.at[k], cnt_rsem.at[k], target)
            copy.start()
            sends.append(copy)

        arrival(zbuf.at[0], 0).wait_recv()
        zbuf[z + 1] = zbuf[0] + mine
        for k, step in ((1, 1), (2, 2), (3, -1), (4, -2)):
            push(zbuf.at[z + 1], at_z(step), k)
        back1, back2 = lax.rem(z + ZS - 1, ZS), lax.rem(z + ZS - 2, ZS)
        ahead1, ahead2 = lax.rem(z + 1, ZS), lax.rem(z + 2, ZS)
        back3, back4, ahead3 = lax.rem(z + ZS - 3, ZS), lax.rem(z + ZS - 4, ZS), lax.rem(z + 3, ZS)
        for k, slot in ((1, back1), (2, back2), (3, ahead1), (4, ahead2)):
            arrival(zbuf.at[slot + 1], k).wait_recv()
        push(zbuf.at[back2 + 1], at_z(1), 5)
        push(zbuf.at[back2 + 1], at_z(2), 6)
        push(zbuf.at[ahead2 + 1], at_z(-1), 7)
        for k, slot in ((5, back3), (6, back4), (7, ahead3)):
            arrival(zbuf.at[slot + 1], k).wait_recv()
        column = zbuf[1]
        below = jnp.where(z > 0, zbuf[1], 0)
        for i in range(1, ZS):
            column = column + zbuf[i + 1]
            below = below + jnp.where(z > i, zbuf[i + 1], 0)
        xbuf[x] = column
        for step in (1, 2, 3):
            push(xbuf.at[x], at_x(step), 7 + step)
        for step in (1, 2, 3):
            arrival(xbuf.at[lax.rem(x + XS - step, XS)], 7 + step).wait_recv()
        plane = xbuf[0]
        below = below + jnp.where(x > 0, xbuf[0], 0)
        for i in range(1, XS):
            plane = plane + xbuf[i]
            below = below + jnp.where(x > i, xbuf[i], 0)
        ybuf[y] = plane
        for step in (1, 2, 3):
            push(ybuf.at[y], at_y(step), 10 + step)
        for step in (1, 2, 3):
            arrival(ybuf.at[lax.rem(y + YS - step, YS)], 10 + step).wait_recv()
        for i in range(YS):
            below = below + jnp.where(y > i, ybuf[i], 0)
        ebuf[0] = below - me * QROWS
        ebuf[1] = below + mine - (me + 1) * QROWS
        copy = remote(ebuf.at[pl.ds(0, 2)], ebuf.at[pl.ds(2, 2)], cnt_ssem.at[14], cnt_rsem.at[14], me + 1)
        copy.start()
        sends.append(copy)
        place[0] = ebuf[0]
        place[1] = jnp.full_like(ebuf[0], -1)

        for g in order:
            @pl.when(me > 0)
            def _(g=g):
                remote(send[g], near_at(g), cross_ssem.at[g], near_rsem.at[g], me + 1).wait_recv()

            piece = nearx.at[:, pl.ds(QROWS, WIN)] if g == groups else near.at[pl.ds(g * rows, rows), pl.ds(QROWS, WIN)]
            copy = remote(piece, far_at(g), far_ssem.at[g], far_rsem.at[g], me + 1)
            copy.start()
            sends.append(copy)
        for copy in sends:
            copy.wait_send()
        for g in order:
            remote(ends[g], near_at(g), near_ssem.at[g], near_rsem.at[g], me + 1).wait_send()

    @pl.when(odd)
    def _():
        remote(ebuf.at[pl.ds(0, 2)], ebuf.at[pl.ds(2, 2)], cnt_ssem.at[14], cnt_rsem.at[14], me - 1).wait_recv()
        place[0] = ebuf[3]
        place[1] = ebuf[2] - (QROWS - WIN)
        for g in order:
            remote(far_at(g), far_at(g), far_ssem.at[g], far_rsem.at[g], me - 1).wait_recv()
        remote(pairin, zbuf.at[0], cnt_ssem.at[0], cnt_rsem.at[0], me - 1).wait_send()

        @pl.when(jnp.logical_not(last))
        def _():
            for g in order:
                remote(send[g], near_at(g), cross_ssem.at[g], near_rsem.at[g], me + 1).wait_send()


def exchange(counts, returns, xw, groups):
    stocks = returns.shape[0]
    rows = stocks // groups
    bf = jnp.bfloat16

    def per(length):
        return [pltpu.VMEM((rows, length), bf)] * groups + [pltpu.VMEM((2, length), bf)]

    n = groups + 1
    dma = pltpu.SemaphoreType.DMA
    row = lambda k: pltpu.VMEM((k, 1, LANES), jnp.int32)
    vmem = pl.BlockSpec(memory_space=pltpu.VMEM)
    smem = pl.BlockSpec(memory_space=pltpu.SMEM)
    shape = jax.ShapeDtypeStruct
    return pl.pallas_call(
        functools.partial(exchange_kernel, groups, rows),
        out_shape=(shape((stocks, REACH), bf), shape((stocks, WIN), bf), shape((2, REACH), bf), shape((2, WIN), bf), shape((2, 1, LANES), jnp.int32)),
        in_specs=[smem, vmem, vmem],
        out_specs=(vmem,) * 5,
        scratch_shapes=per(REACH) + per(REACH)
        + [pltpu.VMEM((OT, rows, LANES), bf)] * groups + [pltpu.VMEM((OT, 2, LANES), bf)]
        + [pltpu.VMEM((1, LANES), jnp.int32), row(ZS + 1), row(XS), row(YS), row(4)]
        + [dma((n,)), dma((n,)), dma((n,)), dma((n,)), dma((n,)), dma((15,)), dma((15,))],
        compiler_params=pltpu.CompilerParams(collective_id=0, has_side_effects=True, vmem_limit_bytes=40 << 20),
        name="exchange",
    )(counts, returns, xw)


def slope_kernel(rows, place, near, far, own, nearx, farx, xw, out, pre, suf, stats, wx):
    tiles = REACH // TILE
    halo = WIN // TILE
    outs = tiles - halo
    cut = lambda a, t: a[:, t * TILE : (t + 1) * TILE]
    excess = jnp.max(place[0])
    edge = jnp.max(place[1])

    def aligned(near, far, own):
        m = own.shape[0]
        def load(k):
            return jnp.where(k < RT, clamped(near, 0, m, k), clamped(own, 0, m, k - RT))

        parts = rolled(load, QROWS - excess, RT, m)
        older = rolled(lambda k: clamped(far, 0, m, k), WIN - jnp.maximum(edge, 0), TT, m)
        lane = lax.broadcasted_iota(jnp.int32, (m, LANES), 1)
        for j in range(TT):
            parts[j] = jnp.where(lane < edge - j * LANES, older[j], parts[j])
        return jnp.concatenate(parts, 1)

    def sums(a):
        m = a.shape[0]
        stack = jnp.concatenate([cut(a, t) for t in range(tiles)], 0)
        head = jnp.dot(stack, pre[...], preferred_element_type=jnp.float32)
        tail = jnp.dot(stack[: outs * m], suf[...], preferred_element_type=jnp.float32)
        whole = [head[t * m : (t + 1) * m, TILE - 1 :] for t in range(tiles)]
        result = []
        for t in range(halo, tiles):
            between = whole[t - 3] + whole[t - 2] + whole[t - 1]
            s = t - halo
            result.append(head[t * m : (t + 1) * m] + tail[s * m : (s + 1) * m] + between)
        return result

    @pl.when(pl.program_id(0) == 0)
    def _():
        q = lax.broadcasted_iota(jnp.int32, (TILE, TILE), 0)
        p = lax.broadcasted_iota(jnp.int32, (TILE, TILE), 1)
        pre[...] = jnp.where(q <= p, 1.0, 0.0).astype(jnp.bfloat16)
        suf[...] = jnp.where(q > p, 1.0, 0.0).astype(jnp.bfloat16)
        wx[...] = aligned(nearx, farx, xw)
        xf = wx[0:1, :].astype(jnp.float32)
        wf = wx[1:2, :].astype(jnp.float32)
        row = lax.broadcasted_iota(jnp.int32, (16, REACH), 0)
        a = jnp.where(row == 0, wf, jnp.where(row == 1, xf, xf * xf)).astype(jnp.bfloat16)
        for i, s in enumerate(sums(a)):
            sw, sx, sxx = s[0:1], s[1:2], s[2:3]
            stats[0:1, i * TILE : (i + 1) * TILE] = sw
            stats[1:2, i * TILE : (i + 1) * TILE] = sx
            stats[2:3, i * TILE : (i + 1) * TILE] = 1.0 / (sw * sxx - sx * sx + RIDGE * WIN * WIN)

    x = wx[0:1, :]
    w = wx[1:2, :]
    yv = aligned(near, far, own) * w
    cross = (x.astype(jnp.float32) * yv.astype(jnp.float32)).astype(jnp.bfloat16)
    both = sums(jnp.concatenate([cross, yv], 0))
    for i, s in enumerate(both):
        c = slice(i * TILE, (i + 1) * TILE)
        out[:, c] = (stats[0:1, c] * s[:rows] - stats[1:2, c] * s[rows:]) * stats[2:3, c]


def slopes(place, near, far, own, nearx, farx, xw, rows):
    stocks = near.shape[0]
    block = lambda length: pl.BlockSpec((rows, length), lambda i: (i, 0))
    fixed = lambda length: pl.BlockSpec((2, length), lambda i: (0, 0))
    return pl.pallas_call(
        functools.partial(slope_kernel, rows),
        grid=(stocks // rows,),
        out_shape=jax.ShapeDtypeStruct((stocks, QROWS), jnp.float32),
        in_specs=[pl.BlockSpec(memory_space=pltpu.VMEM), block(REACH), block(WIN), block(CAP), fixed(REACH), fixed(WIN), fixed(CAP)],
        out_specs=block(QROWS),
        scratch_shapes=[
            pltpu.VMEM((TILE, TILE), jnp.bfloat16),
            pltpu.VMEM((TILE, TILE), jnp.bfloat16),
            pltpu.VMEM((8, QROWS), jnp.float32),
            pltpu.VMEM((2, REACH), jnp.bfloat16),
        ],
        compiler_params=pltpu.CompilerParams(dimension_semantics=("arbitrary",), vmem_limit_bytes=40 << 20),
        name="slopes",
    )(place, near, far, own, nearx, farx, xw)


def per_device(returns, market, mask, counts):
    weight = mask.astype(jnp.float32)
    xw = jnp.stack([market.astype(jnp.float32) * weight, weight], 0).astype(jnp.bfloat16)
    near, far, nearx, farx, place = exchange(counts, returns, xw, 8)
    return slopes(place, near, far, returns, nearx, farx, xw, 32)


def solution(mesh):
    return jax.shard_map(
        per_device,
        mesh=mesh,
        in_specs=(P(None, "span"), P("span"), P("span"), P("span")),
        out_specs=P(None, "span"),
        check_vma=False,
    )
```

```python
import functools

import jax
import jax.numpy as jnp
from jax import lax
from jax.experimental import pallas as pl
from jax.experimental.pallas import tpu as pltpu
from jax.sharding import PartitionSpec as P

WIN = 1024
QROWS = 4096
CAP = 2 * QROWS
REACH = QROWS + WIN
RIDGE = 0.1
LANES = 128
TILE = 256
RT = REACH // LANES
OT = CAP // LANES
TT = WIN // LANES
MESH = pl.DeviceIdType.MESH
ZS, XS, YS = 8, 4, 4


def rolled(load, start, tiles, rows):
    first = lax.shift_right_logical(start, 7)
    r = jnp.bitwise_and(start, LANES - 1)
    turn = jnp.bitwise_and(LANES - r, LANES - 1)
    keep = lax.broadcasted_iota(jnp.int32, (rows, LANES), 1) < LANES - r
    turned = [pltpu.roll(load(first + j), turn, 1) for j in range(tiles + 1)]
    return [jnp.where(keep, turned[j], turned[j + 1]) for j in range(tiles)]


def moved_right(tiles, ticks, count):
    r = jnp.bitwise_and(ticks, LANES - 1)
    turned = [pltpu.roll(tile, r, 1) for tile in tiles]
    low = lax.broadcasted_iota(jnp.int32, tiles[0].shape, 1) < r
    n = len(tiles)
    at = {i: jnp.where(low, turned[max(i - 1, 0)], turned[min(i, n - 1)]) for i in range(n + 1)}
    for bit in (32, 16, 8, 4, 2, 1):
        taken = jnp.bitwise_and(ticks, bit * LANES) != 0
        moved = {}
        for i in range(count):
            if i in at and i - bit in at:
                moved[i] = jnp.where(taken, at[i - bit], at[i])
            elif i in at or i - bit in at:
                moved[i] = at[i] if i in at else at[i - bit]
        at = moved
    return at


def aligned(tiles, far_tiles, excess, edge):
    m = tiles.shape[1]
    parts = rolled(lambda k: tiles[jnp.minimum(jnp.maximum(k, 0), RT + OT - 1)], QROWS - excess, RT, m)
    older = rolled(lambda k: far_tiles[jnp.minimum(jnp.maximum(k, 0), TT - 1)], WIN - jnp.maximum(edge, 0), TT, m)
    lane = lax.broadcasted_iota(jnp.int32, (m, LANES), 1)
    for j in range(TT):
        parts[j] = jnp.where(lane < edge - j * LANES, older[j], parts[j])
    return jnp.concatenate(parts, 1)


def window_sums(a, pre, suf):
    m = a.shape[0]
    tiles, halo = REACH // TILE, WIN // TILE
    stack = jnp.concatenate([a[:, t * TILE : (t + 1) * TILE] for t in range(tiles)], 0)
    head = jnp.dot(stack, pre[...], preferred_element_type=jnp.float32)
    tail = jnp.dot(stack[: (tiles - halo) * m], suf[...], preferred_element_type=jnp.float32)
    whole = [head[t * m : (t + 1) * m, TILE - 1 :] for t in range(tiles)]
    result = []
    for t in range(halo, tiles):
        between = whole[t - 3] + whole[t - 2] + whole[t - 1]
        s = t - halo
        result.append(head[t * m : (t + 1) * m] + tail[s * m : (s + 1) * m] + between)
    return result


def span_kernel(sizes, counts, returns, market_in, mask_in, out, *scratch):
    groups = len(sizes)
    starts = [sum(sizes[:g]) for g in range(groups)]
    n = groups + 1
    it = iter(scratch)
    take = lambda k=n: [next(it) for _ in range(k)]
    ends, send, near, far, tiled, fars = take(), take(), take(), take(), take(), take()
    own = take(groups)
    pairin, zbuf, xbuf, ybuf, ebuf, place = take(6)
    pre, suf, stats, wx, market, mask = take(6)
    own_sem, near_ssem, cross_ssem, near_rsem, far_ssem, far_rsem, cnt_ssem, cnt_rsem = take(8)

    me = lax.axis_index("span")
    total = ZS * XS * YS * 2
    even = lax.rem(me, 2) == 0
    odd = lax.rem(me, 2) == 1
    last = me == total - 1
    chip = lax.div(me, 2)
    z = lax.rem(chip, ZS)
    x = lax.rem(lax.div(chip, ZS), XS)
    y = lax.div(chip, ZS * XS)

    def core0(yy, xx, zz):
        return ((yy * XS + xx) * ZS + zz) * 2

    def at_z(step):
        return core0(y, x, lax.rem(z + step + ZS, ZS))

    def at_x(step):
        return core0(y, lax.rem(x + step, XS), z)

    def at_y(step):
        return core0(lax.rem(y + step, YS), x, z)

    order = [groups] + list(range(groups))

    def remote(src, dst, ssem, rsem, target):
        return pltpu.make_async_remote_copy(
            src_ref=src, dst_ref=dst, send_sem=ssem, recv_sem=rsem, device_id=(target,), device_id_type=MESH
        )

    series = [
        pltpu.make_async_copy(market_in, market, own_sem.at[groups]),
        pltpu.make_async_copy(mask_in, mask, own_sem.at[n]),
    ]
    for load in series:
        load.start()
    loads = []
    for g in range(groups):
        load = pltpu.make_async_copy(returns.at[pl.ds(starts[g], sizes[g]), :], own[g], own_sem.at[g])
        load.start()
        loads.append(load)

    barrier = pltpu.get_barrier_semaphore()

    def hello(target):
        pl.semaphore_signal(barrier, inc=1, device_id=(target,), device_id_type=MESH)

    mine = counts[0]

    @pl.when(even)
    def _():
        hello(me + 1)

        @pl.when(me > 0)
        def _():
            hello(me - 1)

        for step in (1, 2, -1, -2):
            hello(at_z(step))
        for step in (1, 2, 3):
            hello(at_x(step))
            hello(at_y(step))

    @pl.when(odd)
    def _():
        hello(me - 1)

        @pl.when(jnp.logical_not(last))
        def _():
            hello(me + 1)

    pairin[...] = jnp.zeros_like(pairin) + mine

    @pl.when(me == 0)
    def _():
        for g in order:
            near[g][...] = jnp.zeros_like(near[g])

    def end_window(g):
        m = ends[g].shape[0]
        if g == groups:
            for load in series:
                load.wait()
            w = mask[...].astype(jnp.float32)
            v = market[...].astype(jnp.float32) * w
            for t in range(OT):
                tiled[g][RT + t] = jnp.concatenate([v[t : t + 1], w[t : t + 1]], 0).astype(jnp.bfloat16)
        else:
            loads[g].wait()
            for t in range(OT):
                tiled[g][RT + t] = own[g][:, t * LANES : (t + 1) * LANES]
        slot = lambda k: tiled[g][jnp.minimum(jnp.maximum(k, RT), RT + OT - 1)]
        for j, value in enumerate(rolled(slot, mine, RT, m)):
            ends[g][:, j * LANES : (j + 1) * LANES] = value

    def cross(g):
        @pl.when(odd)
        def _():
            remote(ends[g], near[g], near_ssem.at[g], near_rsem.at[g], me - 1).wait_recv()
            short = jnp.maximum(REACH - mine, 0)

            @pl.when(jnp.logical_not(last))
            def _():
                m = ends[g].shape[0]
                for first in range(0, m, 16):
                    part = min(m, 16)
                    b = slice(first, first + part)
                    tail = [near[g][b, QROWS + j * LANES : QROWS + (j + 1) * LANES] for j in range(TT)]
                    placed = moved_right(tail, short, RT + TT)
                    lane = lax.broadcasted_iota(jnp.int32, (part, LANES), 1)
                    for j in range(RT):
                        c = slice(j * LANES, (j + 1) * LANES)
                        send[g][b, c] = jnp.where(lane < short - j * LANES, placed[j + TT], ends[g][b, c])
                remote(send[g], near[g], cross_ssem.at[g], near_rsem.at[g], me + 1).start()

    def to_partner(g):
        @pl.when(even)
        def _():
            remote(ends[g], near[g], near_ssem.at[g], near_rsem.at[g], me + 1).start()

    end_window(order[0])
    end_window(order[1])

    @pl.when(even)
    def _():
        pl.semaphore_wait(barrier, 11 + jnp.where(me > 0, 1, 0))

    @pl.when(odd)
    def _():
        pl.semaphore_wait(barrier, 2 - jnp.where(last, 1, 0))
        remote(pairin, zbuf.at[0], cnt_ssem.at[0], cnt_rsem.at[0], me - 1).start()

    to_partner(order[0])
    to_partner(order[1])
    for i in range(2, n):
        end_window(order[i])
        to_partner(order[i])
        cross(order[i - 2])
    cross(order[n - 2])
    cross(order[n - 1])

    q = lax.broadcasted_iota(jnp.int32, (TILE, TILE), 0)
    p = lax.broadcasted_iota(jnp.int32, (TILE, TILE), 1)
    pre[...] = jnp.where(q <= p, 1.0, 0.0).astype(jnp.bfloat16)
    suf[...] = jnp.where(q > p, 1.0, 0.0).astype(jnp.bfloat16)

    @pl.when(even)
    def _():
        def arrival(dst, k):
            return remote(dst, dst, cnt_ssem.at[k], cnt_rsem.at[k], me + 1)

        sends = []

        def push(ref, target, k):
            copy = remote(ref, ref, cnt_ssem.at[k], cnt_rsem.at[k], target)
            copy.start()
            sends.append(copy)

        arrival(zbuf.at[0], 0).wait_recv()
        zbuf[z + 1] = zbuf[0] + mine
        for k, step in ((1, 1), (2, 2), (3, -1), (4, -2)):
            push(zbuf.at[z + 1], at_z(step), k)
        back1, back2 = lax.rem(z + ZS - 1, ZS), lax.rem(z + ZS - 2, ZS)
        ahead1, ahead2 = lax.rem(z + 1, ZS), lax.rem(z + 2, ZS)
        back3, back4, ahead3 = lax.rem(z + ZS - 3, ZS), lax.rem(z + ZS - 4, ZS), lax.rem(z + 3, ZS)
        for k, slot in ((1, back1), (2, back2), (3, ahead1), (4, ahead2)):
            arrival(zbuf.at[slot + 1], k).wait_recv()
        push(zbuf.at[back2 + 1], at_z(1), 5)
        push(zbuf.at[back2 + 1], at_z(2), 6)
        push(zbuf.at[ahead2 + 1], at_z(-1), 7)
        for k, slot in ((5, back3), (6, back4), (7, ahead3)):
            arrival(zbuf.at[slot + 1], k).wait_recv()
        column = zbuf[1]
        below = jnp.where(z > 0, zbuf[1], 0)
        for i in range(1, ZS):
            column = column + zbuf[i + 1]
            below = below + jnp.where(z > i, zbuf[i + 1], 0)
        xbuf[x] = column
        for step in (1, 2, 3):
            push(xbuf.at[x], at_x(step), 7 + step)
        for step in (1, 2, 3):
            arrival(xbuf.at[lax.rem(x + XS - step, XS)], 7 + step).wait_recv()
        plane = xbuf[0]
        below = below + jnp.where(x > 0, xbuf[0], 0)
        for i in range(1, XS):
            plane = plane + xbuf[i]
            below = below + jnp.where(x > i, xbuf[i], 0)
        ybuf[y] = plane
        for step in (1, 2, 3):
            push(ybuf.at[y], at_y(step), 10 + step)
        for step in (1, 2, 3):
            arrival(ybuf.at[lax.rem(y + YS - step, YS)], 10 + step).wait_recv()
        for i in range(YS):
            below = below + jnp.where(y > i, ybuf[i], 0)
        ebuf[0] = below - me * QROWS
        ebuf[1] = below + mine - (me + 1) * QROWS
        copy = remote(ebuf.at[pl.ds(0, 2)], ebuf.at[pl.ds(2, 2)], cnt_ssem.at[14], cnt_rsem.at[14], me + 1)
        copy.start()
        sends.append(copy)
        place[0] = ebuf[0]
        place[1] = jnp.full_like(ebuf[0], -1)
        for copy in sends:
            copy.wait_send()

    @pl.when(odd)
    def _():
        remote(ebuf.at[pl.ds(0, 2)], ebuf.at[pl.ds(2, 2)], cnt_ssem.at[14], cnt_rsem.at[14], me - 1).wait_recv()
        place[0] = ebuf[3]
        place[1] = ebuf[2] - (QROWS - WIN)

    excess = jnp.max(place[0])
    edge = jnp.max(place[1])
    for g in order:
        piece = near[g].at[:, pl.ds(QROWS, WIN)]

        @pl.when(even)
        def _():
            @pl.when(me > 0)
            def _():
                remote(send[g], near[g], cross_ssem.at[g], near_rsem.at[g], me + 1).wait_recv()

            remote(piece, far[g], far_ssem.at[g], far_rsem.at[g], me + 1).start()

        for t in range(RT):
            tiled[g][t] = near[g][:, t * LANES : (t + 1) * LANES]

        @pl.when(odd)
        def _():
            remote(piece, far[g], far_ssem.at[g], far_rsem.at[g], me - 1).wait_recv()
            for t in range(TT):
                fars[g][t] = far[g][:, t * LANES : (t + 1) * LANES]

        ticks = aligned(tiled[g], fars[g], excess, edge)
        if g == groups:
            wx[...] = ticks
            xf = ticks[0:1, :].astype(jnp.float32)
            wf = ticks[1:2, :].astype(jnp.float32)
            row = lax.broadcasted_iota(jnp.int32, (16, REACH), 0)
            a = jnp.where(row == 0, wf, jnp.where(row == 1, xf, xf * xf)).astype(jnp.bfloat16)
            for i, s in enumerate(window_sums(a, pre, suf)):
                c = slice(i * TILE, (i + 1) * TILE)
                sw, sx, sxx = s[0:1], s[1:2], s[2:3]
                stats[0:1, c] = sw
                stats[1:2, c] = sx
                stats[2:3, c] = 1.0 / (sw * sxx - sx * sx + RIDGE * WIN * WIN)
        else:
            m = sizes[g]
            yv = ticks * wx[1:2, :]
            crossed = (wx[0:1, :].astype(jnp.float32) * yv.astype(jnp.float32)).astype(jnp.bfloat16)
            for i, s in enumerate(window_sums(jnp.concatenate([crossed, yv], 0), pre, suf)):
                c = slice(i * TILE, (i + 1) * TILE)
                value = (stats[0:1, c] * s[:m] - stats[1:2, c] * s[m:]) * stats[2:3, c]
                out[starts[g] : starts[g] + m, c] = value

    @pl.when(even)
    def _():
        for g in order:
            remote(ends[g], near[g], near_ssem.at[g], near_rsem.at[g], me + 1).wait_send()
            remote(near[g].at[:, pl.ds(QROWS, WIN)], far[g], far_ssem.at[g], far_rsem.at[g], me + 1).wait_send()

    @pl.when(odd)
    def _():
        remote(pairin, zbuf.at[0], cnt_ssem.at[0], cnt_rsem.at[0], me - 1).wait_send()

        @pl.when(jnp.logical_not(last))
        def _():
            for g in order:
                remote(send[g], near[g], cross_ssem.at[g], near_rsem.at[g], me + 1).wait_send()


def slopes(counts, returns, market, mask, sizes):
    stocks = returns.shape[0]
    bf = jnp.bfloat16

    def per(shape):
        return [pltpu.VMEM(shape(m), bf) for m in list(sizes) + [2]]

    flat = lambda length: per(lambda m: (m, length))
    split = lambda count: per(lambda m: (count, m, LANES))
    n = len(sizes) + 1
    dma = pltpu.SemaphoreType.DMA
    row = lambda k: pltpu.VMEM((k, 1, LANES), jnp.int32)
    vmem = pl.BlockSpec(memory_space=pltpu.VMEM)
    return pl.pallas_call(
        functools.partial(span_kernel, sizes),
        out_shape=jax.ShapeDtypeStruct((stocks, QROWS), jnp.float32),
        in_specs=[pl.BlockSpec(memory_space=pltpu.SMEM)] + [pl.BlockSpec(memory_space=pltpu.HBM)] * 3,
        out_specs=vmem,
        scratch_shapes=flat(REACH) + flat(REACH) + flat(REACH) + flat(WIN) + split(RT + OT) + split(TT)
        + flat(CAP)[:-1]
        + [pltpu.VMEM((1, LANES), jnp.int32), row(ZS + 1), row(XS), row(YS), row(4), row(2)]
        + [pltpu.VMEM((TILE, TILE), bf)] * 2
        + [pltpu.VMEM((8, QROWS), jnp.float32), pltpu.VMEM((2, REACH), bf)]
        + [pltpu.VMEM((OT, LANES), bf), pltpu.VMEM((OT, LANES), jnp.int32)]
        + [dma((n + 1,))] * 6 + [dma((15,))] * 2,
        compiler_params=pltpu.CompilerParams(collective_id=0, has_side_effects=True, vmem_limit_bytes=48 << 20),
        name="slopes",
    )(counts, returns, market, mask)


def per_device(returns, market, mask, counts):
    sizes = (32,) * 8
    return slopes(counts, returns, market.reshape(OT, LANES), mask.reshape(OT, LANES), sizes)


def solution(mesh):
    return jax.shard_map(
        per_device,
        mesh=mesh,
        in_specs=(P(None, "span"), P("span"), P("span"), P("span")),
        out_specs=P(None, "span"),
        check_vma=False,
    )
```

```python
import functools

import jax
import jax.numpy as jnp
from jax import lax
from jax.experimental import pallas as pl
from jax.experimental.pallas import tpu as pltpu
from jax.sharding import PartitionSpec as P

WIN = 1024
QROWS = 4096
CAP = 2 * QROWS
REACH = QROWS + WIN
RIDGE = 0.1
LANES = 128
TILE = 256
RT = REACH // LANES
OT = CAP // LANES
TT = WIN // LANES
MESH = pl.DeviceIdType.MESH
ZS, XS, YS = 8, 4, 4


def rolled(load, start, tiles, rows):
    first = lax.shift_right_logical(start, 7)
    r = jnp.bitwise_and(start, LANES - 1)
    turn = jnp.bitwise_and(LANES - r, LANES - 1)
    keep = lax.broadcasted_iota(jnp.int32, (rows, LANES), 1) < LANES - r
    turned = [pltpu.roll(load(first + j), turn, 1) for j in range(tiles + 1)]
    return [jnp.where(keep, turned[j], turned[j + 1]) for j in range(tiles)]


def moved_right(tiles, ticks, count):
    r = jnp.bitwise_and(ticks, LANES - 1)
    turned = [pltpu.roll(tile, r, 1) for tile in tiles]
    low = lax.broadcasted_iota(jnp.int32, tiles[0].shape, 1) < r
    n = len(tiles)
    at = {i: jnp.where(low, turned[max(i - 1, 0)], turned[min(i, n - 1)]) for i in range(n + 1)}
    for bit in (32, 16, 8, 4, 2, 1):
        taken = jnp.bitwise_and(ticks, bit * LANES) != 0
        moved = {}
        for i in range(count):
            if i in at and i - bit in at:
                moved[i] = jnp.where(taken, at[i - bit], at[i])
            elif i in at or i - bit in at:
                moved[i] = at[i] if i in at else at[i - bit]
        at = moved
    return at


def aligned(tiles, far_tiles, excess, edge):
    m = tiles.shape[1]
    parts = rolled(lambda k: tiles[jnp.minimum(jnp.maximum(k, 0), RT + OT - 1)], QROWS - excess, RT, m)
    older = rolled(lambda k: far_tiles[jnp.minimum(jnp.maximum(k, 0), TT - 1)], WIN - jnp.maximum(edge, 0), TT, m)
    lane = lax.broadcasted_iota(jnp.int32, (m, LANES), 1)
    for j in range(TT):
        parts[j] = jnp.where(lane < edge - j * LANES, older[j], parts[j])
    return jnp.concatenate(parts, 1)


def window_sums(a, pre, suf):
    m = a.shape[0]
    tiles, halo = REACH // TILE, WIN // TILE
    stack = jnp.concatenate([a[:, t * TILE : (t + 1) * TILE] for t in range(tiles)], 0)
    head = jnp.dot(stack, pre[...], preferred_element_type=jnp.float32)
    tail = jnp.dot(stack[: (tiles - halo) * m], suf[...], preferred_element_type=jnp.float32)
    whole = [head[t * m : (t + 1) * m, TILE - 1 :] for t in range(tiles)]
    result = []
    for t in range(halo, tiles):
        between = whole[t - 3] + whole[t - 2] + whole[t - 1]
        s = t - halo
        result.append(head[t * m : (t + 1) * m] + tail[s * m : (s + 1) * m] + between)
    return result


def span_kernel(sizes, counts, returns, market_in, mask_in, out, *scratch):
    groups = len(sizes)
    starts = [sum(sizes[:g]) for g in range(groups)]
    n = groups + 1
    it = iter(scratch)
    take = lambda k=n: [next(it) for _ in range(k)]
    ends, send, near, far, tiled, fars = take(), take(), take(), take(), take(), take()
    own = take(groups)
    pairin, zbuf, xbuf, ybuf, ebuf, place = take(6)
    pre, suf, stats, wx, market, mask = take(6)
    own_sem, near_ssem, cross_ssem, near_rsem, far_ssem, far_rsem, cnt_ssem, cnt_rsem, present = take(9)

    me = lax.axis_index("span")
    total = ZS * XS * YS * 2
    even = lax.rem(me, 2) == 0
    odd = lax.rem(me, 2) == 1
    last = me == total - 1
    chip = lax.div(me, 2)
    z = lax.rem(chip, ZS)
    x = lax.rem(lax.div(chip, ZS), XS)
    y = lax.div(chip, ZS * XS)

    def core0(yy, xx, zz):
        return ((yy * XS + xx) * ZS + zz) * 2

    def at_z(step):
        return core0(y, x, lax.rem(z + step + ZS, ZS))

    def at_x(step):
        return core0(y, lax.rem(x + step, XS), z)

    def at_y(step):
        return core0(lax.rem(y + step, YS), x, z)

    order = [groups] + list(range(groups))

    def remote(src, dst, ssem, rsem, target):
        return pltpu.make_async_remote_copy(
            src_ref=src, dst_ref=dst, send_sem=ssem, recv_sem=rsem, device_id=(target,), device_id_type=MESH
        )

    series = [
        pltpu.make_async_copy(market_in, market, own_sem.at[groups]),
        pltpu.make_async_copy(mask_in, mask, own_sem.at[n]),
    ]
    for load in series:
        load.start()
    loads = []
    for g in range(groups):
        load = pltpu.make_async_copy(returns.at[pl.ds(starts[g], sizes[g]), :], own[g], own_sem.at[g])
        load.start()
        loads.append(load)

    barrier = pltpu.get_barrier_semaphore()

    def hello(target):
        pl.semaphore_signal(barrier, inc=1, device_id=(target,), device_id_type=MESH)

    mine = counts[0]

    @pl.when(even)
    def _():
        hello(me + 1)

        @pl.when(me > 0)
        def _():
            hello(me - 1)

        for step in (1, 2, -1, -2):
            hello(at_z(step))
        for step in (1, 2, 3):
            hello(at_x(step))
            hello(at_y(step))

    pairin[...] = jnp.zeros_like(pairin) + mine

    @pl.when(me == 0)
    def _():
        for g in order:
            near[g][...] = jnp.zeros_like(near[g])

    def end_window(g):
        m = ends[g].shape[0]
        if g == groups:
            for load in series:
                load.wait()
            w = mask[...].astype(jnp.float32)
            v = market[...].astype(jnp.float32) * w
            for t in range(OT):
                tiled[g][RT + t] = jnp.concatenate([v[t : t + 1], w[t : t + 1]], 0).astype(jnp.bfloat16)
        else:
            loads[g].wait()
            for t in range(OT):
                tiled[g][RT + t] = own[g][:, t * LANES : (t + 1) * LANES]
        slot = lambda k: tiled[g][jnp.minimum(jnp.maximum(k, RT), RT + OT - 1)]
        for j, value in enumerate(rolled(slot, mine, RT, m)):
            ends[g][:, j * LANES : (j + 1) * LANES] = value

    def cross(g):
        @pl.when(odd)
        def _():
            remote(ends[g], near[g], near_ssem.at[g], near_rsem.at[g], me - 1).wait_recv()
            short = jnp.maximum(REACH - mine, 0)

            @pl.when(jnp.logical_not(last))
            def _():
                m = ends[g].shape[0]
                for first in range(0, m, 16):
                    part = min(m, 16)
                    b = slice(first, first + part)
                    tail = [near[g][b, QROWS + j * LANES : QROWS + (j + 1) * LANES] for j in range(TT)]
                    placed = moved_right(tail, short, RT + TT)
                    lane = lax.broadcasted_iota(jnp.int32, (part, LANES), 1)
                    for j in range(RT):
                        c = slice(j * LANES, (j + 1) * LANES)
                        send[g][b, c] = jnp.where(lane < short - j * LANES, placed[j + TT], ends[g][b, c])
                remote(send[g], near[g], cross_ssem.at[g], near_rsem.at[g], me + 1).start()

    def to_partner(g):
        @pl.when(even)
        def _():
            remote(ends[g], near[g], near_ssem.at[g], near_rsem.at[g], me + 1).start()

    end_window(order[0])
    end_window(order[1])

    @pl.when(odd)
    def _():
        pl.semaphore_wait(barrier, 2 - jnp.where(last, 1, 0))
        pl.semaphore_signal(present, inc=1, device_id=(me - 1,), device_id_type=MESH)
        remote(pairin, zbuf.at[0], cnt_ssem.at[0], cnt_rsem.at[0], me - 1).start()

    @pl.when(even)
    def _():
        pl.semaphore_wait(present, 1)

    to_partner(order[0])
    to_partner(order[1])
    for i in range(2, n):
        end_window(order[i])
        to_partner(order[i])
        cross(order[i - 2])
    cross(order[n - 2])
    cross(order[n - 1])

    q = lax.broadcasted_iota(jnp.int32, (TILE, TILE), 0)
    p = lax.broadcasted_iota(jnp.int32, (TILE, TILE), 1)
    pre[...] = jnp.where(q <= p, 1.0, 0.0).astype(jnp.bfloat16)
    suf[...] = jnp.where(q > p, 1.0, 0.0).astype(jnp.bfloat16)

    @pl.when(even)
    def _():
        def arrival(dst, k):
            return remote(dst, dst, cnt_ssem.at[k], cnt_rsem.at[k], me + 1)

        sends = []

        def push(ref, target, k):
            copy = remote(ref, ref, cnt_ssem.at[k], cnt_rsem.at[k], target)
            copy.start()
            sends.append(copy)

        pl.semaphore_wait(barrier, 10)
        arrival(zbuf.at[0], 0).wait_recv()
        zbuf[z + 1] = zbuf[0] + mine
        for k, step in ((1, 1), (2, 2), (3, -1), (4, -2)):
            push(zbuf.at[z + 1], at_z(step), k)
        back1, back2 = lax.rem(z + ZS - 1, ZS), lax.rem(z + ZS - 2, ZS)
        ahead1, ahead2 = lax.rem(z + 1, ZS), lax.rem(z + 2, ZS)
        back3, back4, ahead3 = lax.rem(z + ZS - 3, ZS), lax.rem(z + ZS - 4, ZS), lax.rem(z + 3, ZS)
        for k, slot in ((1, back1), (2, back2), (3, ahead1), (4, ahead2)):
            arrival(zbuf.at[slot + 1], k).wait_recv()
        push(zbuf.at[back2 + 1], at_z(1), 5)
        push(zbuf.at[back2 + 1], at_z(2), 6)
        push(zbuf.at[ahead2 + 1], at_z(-1), 7)
        for k, slot in ((5, back3), (6, back4), (7, ahead3)):
            arrival(zbuf.at[slot + 1], k).wait_recv()
        column = zbuf[1]
        below = jnp.where(z > 0, zbuf[1], 0)
        for i in range(1, ZS):
            column = column + zbuf[i + 1]
            below = below + jnp.where(z > i, zbuf[i + 1], 0)
        xbuf[x] = column
        for step in (1, 2, 3):
            push(xbuf.at[x], at_x(step), 7 + step)
        for step in (1, 2, 3):
            arrival(xbuf.at[lax.rem(x + XS - step, XS)], 7 + step).wait_recv()
        plane = xbuf[0]
        below = below + jnp.where(x > 0, xbuf[0], 0)
        for i in range(1, XS):
            plane = plane + xbuf[i]
            below = below + jnp.where(x > i, xbuf[i], 0)
        ybuf[y] = plane
        for step in (1, 2, 3):
            push(ybuf.at[y], at_y(step), 10 + step)
        for step in (1, 2, 3):
            arrival(ybuf.at[lax.rem(y + YS - step, YS)], 10 + step).wait_recv()
        for i in range(YS):
            below = below + jnp.where(y > i, ybuf[i], 0)
        ebuf[0] = below - me * QROWS
        ebuf[1] = below + mine - (me + 1) * QROWS
        copy = remote(ebuf.at[pl.ds(0, 2)], ebuf.at[pl.ds(2, 2)], cnt_ssem.at[14], cnt_rsem.at[14], me + 1)
        copy.start()
        sends.append(copy)
        place[0] = ebuf[0]
        place[1] = jnp.full_like(ebuf[0], -1)
        for copy in sends:
            copy.wait_send()

    @pl.when(odd)
    def _():
        remote(ebuf.at[pl.ds(0, 2)], ebuf.at[pl.ds(2, 2)], cnt_ssem.at[14], cnt_rsem.at[14], me - 1).wait_recv()
        place[0] = ebuf[3]
        place[1] = ebuf[2] - (QROWS - WIN)

    excess = jnp.max(place[0])
    edge = jnp.max(place[1])
    for g in order:
        piece = near[g].at[:, pl.ds(QROWS, WIN)]

        @pl.when(even)
        def _():
            @pl.when(me > 0)
            def _():
                remote(send[g], near[g], cross_ssem.at[g], near_rsem.at[g], me + 1).wait_recv()

            remote(piece, far[g], far_ssem.at[g], far_rsem.at[g], me + 1).start()

        for t in range(RT):
            tiled[g][t] = near[g][:, t * LANES : (t + 1) * LANES]

        @pl.when(odd)
        def _():
            remote(piece, far[g], far_ssem.at[g], far_rsem.at[g], me - 1).wait_recv()
            for t in range(TT):
                fars[g][t] = far[g][:, t * LANES : (t + 1) * LANES]

        ticks = aligned(tiled[g], fars[g], excess, edge)
        if g == groups:
            wx[...] = ticks
            xf = ticks[0:1, :].astype(jnp.float32)
            wf = ticks[1:2, :].astype(jnp.float32)
            row = lax.broadcasted_iota(jnp.int32, (16, REACH), 0)
            a = jnp.where(row == 0, wf, jnp.where(row == 1, xf, xf * xf)).astype(jnp.bfloat16)
            for i, s in enumerate(window_sums(a, pre, suf)):
                c = slice(i * TILE, (i + 1) * TILE)
                sw, sx, sxx = s[0:1], s[1:2], s[2:3]
                stats[0:1, c] = sw
                stats[1:2, c] = sx
                stats[2:3, c] = 1.0 / (sw * sxx - sx * sx + RIDGE * WIN * WIN)
        else:
            m = sizes[g]
            yv = ticks * wx[1:2, :]
            crossed = (wx[0:1, :].astype(jnp.float32) * yv.astype(jnp.float32)).astype(jnp.bfloat16)
            for i, s in enumerate(window_sums(jnp.concatenate([crossed, yv], 0), pre, suf)):
                c = slice(i * TILE, (i + 1) * TILE)
                value = (stats[0:1, c] * s[:m] - stats[1:2, c] * s[m:]) * stats[2:3, c]
                out[starts[g] : starts[g] + m, c] = value

    @pl.when(even)
    def _():
        for g in order:
            remote(ends[g], near[g], near_ssem.at[g], near_rsem.at[g], me + 1).wait_send()
            remote(near[g].at[:, pl.ds(QROWS, WIN)], far[g], far_ssem.at[g], far_rsem.at[g], me + 1).wait_send()

    @pl.when(odd)
    def _():
        remote(pairin, zbuf.at[0], cnt_ssem.at[0], cnt_rsem.at[0], me - 1).wait_send()

        @pl.when(jnp.logical_not(last))
        def _():
            for g in order:
                remote(send[g], near[g], cross_ssem.at[g], near_rsem.at[g], me + 1).wait_send()


def slopes(counts, returns, market, mask, sizes):
    stocks = returns.shape[0]
    bf = jnp.bfloat16

    def per(shape):
        return [pltpu.VMEM(shape(m), bf) for m in list(sizes) + [2]]

    flat = lambda length: per(lambda m: (m, length))
    split = lambda count: per(lambda m: (count, m, LANES))
    n = len(sizes) + 1
    dma = pltpu.SemaphoreType.DMA
    row = lambda k: pltpu.VMEM((k, 1, LANES), jnp.int32)
    vmem = pl.BlockSpec(memory_space=pltpu.VMEM)
    return pl.pallas_call(
        functools.partial(span_kernel, sizes),
        out_shape=jax.ShapeDtypeStruct((stocks, QROWS), jnp.float32),
        in_specs=[pl.BlockSpec(memory_space=pltpu.SMEM)] + [pl.BlockSpec(memory_space=pltpu.HBM)] * 3,
        out_specs=vmem,
        scratch_shapes=flat(REACH) + flat(REACH) + flat(REACH) + flat(WIN) + split(RT + OT) + split(TT)
        + flat(CAP)[:-1]
        + [pltpu.VMEM((1, LANES), jnp.int32), row(ZS + 1), row(XS), row(YS), row(4), row(2)]
        + [pltpu.VMEM((TILE, TILE), bf)] * 2
        + [pltpu.VMEM((8, QROWS), jnp.float32), pltpu.VMEM((2, REACH), bf)]
        + [pltpu.VMEM((OT, LANES), bf), pltpu.VMEM((OT, LANES), jnp.int32)]
        + [dma((n + 1,))] * 6 + [dma((15,))] * 2 + [pltpu.SemaphoreType.REGULAR],
        compiler_params=pltpu.CompilerParams(collective_id=0, has_side_effects=True, vmem_limit_bytes=48 << 20),
        name="slopes",
    )(counts, returns, market, mask)


def per_device(returns, market, mask, counts):
    sizes = (16, 16, 32, 32, 32, 32, 32, 32, 16, 16)
    far = lambda a: pltpu.with_memory_space_constraint(a, pltpu.HBM)
    return slopes(counts, returns, far(market.reshape(OT, LANES)), far(mask.reshape(OT, LANES)), sizes)


def solution(mesh):
    return jax.shard_map(
        per_device,
        mesh=mesh,
        in_specs=(P(None, "span"), P("span"), P("span"), P("span")),
        out_specs=P(None, "span"),
        check_vma=False,
    )
```

```python
import functools

import jax
import jax.numpy as jnp
from jax import lax
from jax.experimental import pallas as pl
from jax.experimental.pallas import tpu as pltpu
from jax.sharding import PartitionSpec as P

WIN = 1024
QROWS = 4096
CAP = 2 * QROWS
REACH = QROWS + WIN
RIDGE = 0.1
LANES = 128
TILE = 256
RT = REACH // LANES
OT = CAP // LANES
TT = WIN // LANES
MESH = pl.DeviceIdType.MESH
ZS, XS, YS = 8, 4, 4


def rolled(load, start, tiles, rows):
    first = lax.shift_right_logical(start, 7)
    r = jnp.bitwise_and(start, LANES - 1)
    turn = jnp.bitwise_and(LANES - r, LANES - 1)
    keep = lax.broadcasted_iota(jnp.int32, (rows, LANES), 1) < LANES - r
    turned = [pltpu.roll(load(first + j), turn, 1) for j in range(tiles + 1)]
    return [jnp.where(keep, turned[j], turned[j + 1]) for j in range(tiles)]


def moved_right(tiles, ticks, count):
    r = jnp.bitwise_and(ticks, LANES - 1)
    turned = [pltpu.roll(tile, r, 1) for tile in tiles]
    low = lax.broadcasted_iota(jnp.int32, tiles[0].shape, 1) < r
    n = len(tiles)
    at = {i: jnp.where(low, turned[max(i - 1, 0)], turned[min(i, n - 1)]) for i in range(n + 1)}
    for bit in (32, 16, 8, 4, 2, 1):
        taken = jnp.bitwise_and(ticks, bit * LANES) != 0
        moved = {}
        for i in range(count):
            if i in at and i - bit in at:
                moved[i] = jnp.where(taken, at[i - bit], at[i])
            elif i in at or i - bit in at:
                moved[i] = at[i] if i in at else at[i - bit]
        at = moved
    return at


def aligned(tiles, far_tiles, excess, edge):
    m = tiles.shape[1]
    parts = rolled(lambda k: tiles[jnp.minimum(jnp.maximum(k, 0), RT + OT - 1)], QROWS - excess, RT, m)
    older = rolled(lambda k: far_tiles[jnp.minimum(jnp.maximum(k, 0), TT - 1)], WIN - jnp.maximum(edge, 0), TT, m)
    lane = lax.broadcasted_iota(jnp.int32, (m, LANES), 1)
    for j in range(TT):
        parts[j] = jnp.where(lane < edge - j * LANES, older[j], parts[j])
    return jnp.concatenate(parts, 1)


def window_sums(a, pre, suf):
    m = a.shape[0]
    tiles, halo = REACH // TILE, WIN // TILE
    stack = jnp.concatenate([a[:, t * TILE : (t + 1) * TILE] for t in range(tiles)], 0)
    head = jnp.dot(stack, pre[...], preferred_element_type=jnp.float32)
    tail = jnp.dot(stack[: (tiles - halo) * m], suf[...], preferred_element_type=jnp.float32)
    whole = [head[t * m : (t + 1) * m, TILE - 1 :] for t in range(tiles)]
    result = []
    for t in range(halo, tiles):
        between = whole[t - 3] + whole[t - 2] + whole[t - 1]
        s = t - halo
        result.append(head[t * m : (t + 1) * m] + tail[s * m : (s + 1) * m] + between)
    return result


def span_kernel(sizes, counts, returns, market_in, mask_in, out, *scratch):
    groups = len(sizes)
    starts = [sum(sizes[:g]) for g in range(groups)]
    n = groups + 1
    it = iter(scratch)
    take = lambda k=n: [next(it) for _ in range(k)]
    ends, send, near, far, tiled, fars = take(), take(), take(), take(), take(), take()
    own = take(groups)
    pairin, zbuf, xbuf, ybuf, ebuf, place = take(6)
    pre, suf, stats, wx, market, mask = take(6)
    own_sem, near_ssem, cross_ssem, near_rsem, far_ssem, far_rsem, cnt_ssem, cnt_rsem, present, ready = take(10)

    me = lax.axis_index("span")
    total = ZS * XS * YS * 2
    even = lax.rem(me, 2) == 0
    odd = lax.rem(me, 2) == 1
    last = me == total - 1
    chip = lax.div(me, 2)
    z = lax.rem(chip, ZS)
    x = lax.rem(lax.div(chip, ZS), XS)
    y = lax.div(chip, ZS * XS)

    def core0(yy, xx, zz):
        return ((yy * XS + xx) * ZS + zz) * 2

    def at_z(step):
        return core0(y, x, lax.rem(z + step + ZS, ZS))

    def at_x(step):
        return core0(y, lax.rem(x + step, XS), z)

    def at_y(step):
        return core0(lax.rem(y + step, YS), x, z)

    order = [groups] + list(range(groups))

    def remote(src, dst, ssem, rsem, target):
        return pltpu.make_async_remote_copy(
            src_ref=src, dst_ref=dst, send_sem=ssem, recv_sem=rsem, device_id=(target,), device_id_type=MESH
        )

    series = [
        pltpu.make_async_copy(market_in, market, own_sem.at[groups]),
        pltpu.make_async_copy(mask_in, mask, own_sem.at[n]),
    ]
    for load in series:
        load.start()
    loads = []
    for g in range(groups):
        load = pltpu.make_async_copy(returns.at[pl.ds(starts[g], sizes[g]), :], own[g], own_sem.at[g])
        load.start()
        loads.append(load)

    barrier = pltpu.get_barrier_semaphore()

    def hello(target):
        pl.semaphore_signal(barrier, inc=1, device_id=(target,), device_id_type=MESH)

    mine = counts[0]

    @pl.when(even)
    def _():
        hello(me + 1)

        @pl.when(me > 0)
        def _():
            hello(me - 1)

        for step in (1, 2, -1, -2):
            hello(at_z(step))
        for step in (1, 2, 3):
            hello(at_x(step))

            @pl.when(y + step < YS)
            def _(step=step):
                hello(at_y(step))

    pairin[...] = jnp.zeros_like(pairin) + mine

    @pl.when(me == 0)
    def _():
        for g in order:
            near[g][...] = jnp.zeros_like(near[g])

    def end_window(g):
        m = ends[g].shape[0]
        if g == groups:
            for load in series:
                load.wait()
            w = mask[...].astype(jnp.float32)
            v = market[...].astype(jnp.float32) * w
            for t in range(OT):
                tiled[g][RT + t] = jnp.concatenate([v[t : t + 1], w[t : t + 1]], 0).astype(jnp.bfloat16)
        else:
            loads[g].wait()
            for t in range(OT):
                tiled[g][RT + t] = own[g][:, t * LANES : (t + 1) * LANES]
        slot = lambda k: tiled[g][jnp.minimum(jnp.maximum(k, RT), RT + OT - 1)]
        for j, value in enumerate(rolled(slot, mine, RT, m)):
            ends[g][:, j * LANES : (j + 1) * LANES] = value

    def cross(g):
        @pl.when(odd)
        def _():
            remote(ends[g], near[g], near_ssem.at[g], near_rsem.at[g], me - 1).wait_recv()
            short = jnp.maximum(REACH - mine, 0)

            @pl.when(jnp.logical_not(last))
            def _():
                m = ends[g].shape[0]
                for first in range(0, m, 16):
                    part = min(m, 16)
                    b = slice(first, first + part)
                    tail = [near[g][b, QROWS + j * LANES : QROWS + (j + 1) * LANES] for j in range(TT)]
                    placed = moved_right(tail, short, RT + TT)
                    lane = lax.broadcasted_iota(jnp.int32, (part, LANES), 1)
                    for j in range(RT):
                        c = slice(j * LANES, (j + 1) * LANES)
                        send[g][b, c] = jnp.where(lane < short - j * LANES, placed[j + TT], ends[g][b, c])
                remote(send[g], near[g], cross_ssem.at[g], near_rsem.at[g], me + 1).start()

    def to_partner(g):
        @pl.when(even)
        def _():
            remote(ends[g], near[g], near_ssem.at[g], near_rsem.at[g], me + 1).start()

    end_window(order[0])
    end_window(order[1])

    @pl.when(odd)
    def _():
        pl.semaphore_wait(barrier, 2 - jnp.where(last, 1, 0))
        pl.semaphore_signal(present, inc=1, device_id=(me - 1,), device_id_type=MESH)
        remote(pairin, zbuf.at[0], cnt_ssem.at[0], cnt_rsem.at[0], me - 1).start()

    @pl.when(even)
    def _():
        pl.semaphore_wait(present, 1)

    to_partner(order[0])
    to_partner(order[1])
    for i in range(2, n):
        end_window(order[i])
        to_partner(order[i])
        cross(order[i - 2])
    cross(order[n - 2])
    cross(order[n - 1])

    q = lax.broadcasted_iota(jnp.int32, (TILE, TILE), 0)
    p = lax.broadcasted_iota(jnp.int32, (TILE, TILE), 1)
    pre[...] = jnp.where(q <= p, 1.0, 0.0).astype(jnp.bfloat16)
    suf[...] = jnp.where(q > p, 1.0, 0.0).astype(jnp.bfloat16)

    @pl.when(even)
    def _():
        def arrival(dst, k):
            return remote(dst, dst, cnt_ssem.at[k], cnt_rsem.at[k], me + 1)

        sends = []

        def push(ref, target, k):
            copy = remote(ref, ref, cnt_ssem.at[k], cnt_rsem.at[k], target)
            copy.start()
            sends.append(copy)

        pl.semaphore_wait(barrier, 7 + y)
        for step in (1, 2, 3):
            @pl.when(y >= step)
            def _(step=step):
                pl.semaphore_signal(ready, inc=1, device_id=(core0(y - step, x, z),), device_id_type=MESH)

        arrival(zbuf.at[0], 0).wait_recv()
        zbuf[z + 1] = zbuf[0] + mine
        for k, step in ((1, 1), (2, 2), (3, -1), (4, -2)):
            push(zbuf.at[z + 1], at_z(step), k)
        back1, back2 = lax.rem(z + ZS - 1, ZS), lax.rem(z + ZS - 2, ZS)
        ahead1, ahead2 = lax.rem(z + 1, ZS), lax.rem(z + 2, ZS)
        back3, back4, ahead3 = lax.rem(z + ZS - 3, ZS), lax.rem(z + ZS - 4, ZS), lax.rem(z + 3, ZS)
        for k, slot in ((1, back1), (2, back2), (3, ahead1), (4, ahead2)):
            arrival(zbuf.at[slot + 1], k).wait_recv()
        push(zbuf.at[back2 + 1], at_z(1), 5)
        push(zbuf.at[back2 + 1], at_z(2), 6)
        push(zbuf.at[ahead2 + 1], at_z(-1), 7)
        for k, slot in ((5, back3), (6, back4), (7, ahead3)):
            arrival(zbuf.at[slot + 1], k).wait_recv()
        column = zbuf[1]
        below = jnp.where(z > 0, zbuf[1], 0)
        for i in range(1, ZS):
            column = column + zbuf[i + 1]
            below = below + jnp.where(z > i, zbuf[i + 1], 0)
        xbuf[x] = column
        for step in (1, 2, 3):
            push(xbuf.at[x], at_x(step), 7 + step)
        for step in (1, 2, 3):
            arrival(xbuf.at[lax.rem(x + XS - step, XS)], 7 + step).wait_recv()
        plane = xbuf[0]
        below = below + jnp.where(x > 0, xbuf[0], 0)
        for i in range(1, XS):
            plane = plane + xbuf[i]
            below = below + jnp.where(x > i, xbuf[i], 0)
        ybuf[y] = plane
        @pl.when(y < YS - 1)
        def _():
            pl.semaphore_wait(ready, YS - 1 - y)

        for step in (1, 2, 3):
            up = remote(ybuf.at[y], ybuf.at[y], cnt_ssem.at[10 + step], cnt_rsem.at[10 + step], at_y(step))
            pl.when(y + step < YS)(up.start)
        for step in (1, 2, 3):
            @pl.when(y >= step)
            def _(step=step):
                arrival(ybuf.at[y - step], 10 + step).wait_recv()
        for i in range(YS):
            below = below + jnp.where(y > i, ybuf[i], 0)
        ebuf[0] = below - me * QROWS
        ebuf[1] = below + mine - (me + 1) * QROWS
        copy = remote(ebuf.at[pl.ds(0, 2)], ebuf.at[pl.ds(2, 2)], cnt_ssem.at[14], cnt_rsem.at[14], me + 1)
        copy.start()
        sends.append(copy)
        place[0] = ebuf[0]
        place[1] = jnp.full_like(ebuf[0], -1)
        for copy in sends:
            copy.wait_send()
        for step in (1, 2, 3):
            up = remote(ybuf.at[y], ybuf.at[y], cnt_ssem.at[10 + step], cnt_rsem.at[10 + step], at_y(step))
            pl.when(y + step < YS)(up.wait_send)

    @pl.when(odd)
    def _():
        remote(ebuf.at[pl.ds(0, 2)], ebuf.at[pl.ds(2, 2)], cnt_ssem.at[14], cnt_rsem.at[14], me - 1).wait_recv()
        place[0] = ebuf[3]
        place[1] = ebuf[2] - (QROWS - WIN)

    excess = jnp.max(place[0])
    edge = jnp.max(place[1])
    for g in order:
        piece = near[g].at[:, pl.ds(QROWS, WIN)]

        @pl.when(even)
        def _():
            @pl.when(me > 0)
            def _():
                remote(send[g], near[g], cross_ssem.at[g], near_rsem.at[g], me + 1).wait_recv()

            remote(piece, far[g], far_ssem.at[g], far_rsem.at[g], me + 1).start()

        for t in range(RT):
            tiled[g][t] = near[g][:, t * LANES : (t + 1) * LANES]

        @pl.when(odd)
        def _():
            remote(piece, far[g], far_ssem.at[g], far_rsem.at[g], me - 1).wait_recv()
            for t in range(TT):
                fars[g][t] = far[g][:, t * LANES : (t + 1) * LANES]

        ticks = aligned(tiled[g], fars[g], excess, edge)
        if g == groups:
            wx[...] = ticks
            xf = ticks[0:1, :].astype(jnp.float32)
            wf = ticks[1:2, :].astype(jnp.float32)
            row = lax.broadcasted_iota(jnp.int32, (16, REACH), 0)
            a = jnp.where(row == 0, wf, jnp.where(row == 1, xf, xf * xf)).astype(jnp.bfloat16)
            for i, s in enumerate(window_sums(a, pre, suf)):
                c = slice(i * TILE, (i + 1) * TILE)
                sw, sx, sxx = s[0:1], s[1:2], s[2:3]
                stats[0:1, c] = sw
                stats[1:2, c] = sx
                stats[2:3, c] = 1.0 / (sw * sxx - sx * sx + RIDGE * WIN * WIN)
        else:
            m = sizes[g]
            yv = ticks * wx[1:2, :]
            crossed = (wx[0:1, :].astype(jnp.float32) * yv.astype(jnp.float32)).astype(jnp.bfloat16)
            for i, s in enumerate(window_sums(jnp.concatenate([crossed, yv], 0), pre, suf)):
                c = slice(i * TILE, (i + 1) * TILE)
                value = (stats[0:1, c] * s[:m] - stats[1:2, c] * s[m:]) * stats[2:3, c]
                out[starts[g] : starts[g] + m, c] = value

    @pl.when(even)
    def _():
        for g in order:
            remote(ends[g], near[g], near_ssem.at[g], near_rsem.at[g], me + 1).wait_send()
            remote(near[g].at[:, pl.ds(QROWS, WIN)], far[g], far_ssem.at[g], far_rsem.at[g], me + 1).wait_send()

    @pl.when(odd)
    def _():
        remote(pairin, zbuf.at[0], cnt_ssem.at[0], cnt_rsem.at[0], me - 1).wait_send()

        @pl.when(jnp.logical_not(last))
        def _():
            for g in order:
                remote(send[g], near[g], cross_ssem.at[g], near_rsem.at[g], me + 1).wait_send()


def slopes(counts, returns, market, mask, sizes):
    stocks = returns.shape[0]
    bf = jnp.bfloat16

    def per(shape):
        return [pltpu.VMEM(shape(m), bf) for m in list(sizes) + [2]]

    flat = lambda length: per(lambda m: (m, length))
    split = lambda count: per(lambda m: (count, m, LANES))
    n = len(sizes) + 1
    dma = pltpu.SemaphoreType.DMA
    row = lambda k: pltpu.VMEM((k, 1, LANES), jnp.int32)
    vmem = pl.BlockSpec(memory_space=pltpu.VMEM)
    return pl.pallas_call(
        functools.partial(span_kernel, sizes),
        out_shape=jax.ShapeDtypeStruct((stocks, QROWS), jnp.float32),
        in_specs=[pl.BlockSpec(memory_space=pltpu.SMEM)] + [pl.BlockSpec(memory_space=pltpu.HBM)] * 3,
        out_specs=vmem,
        scratch_shapes=flat(REACH) + flat(REACH) + flat(REACH) + flat(WIN) + split(RT + OT) + split(TT)
        + flat(CAP)[:-1]
        + [pltpu.VMEM((1, LANES), jnp.int32), row(ZS + 1), row(XS), row(YS), row(4), row(2)]
        + [pltpu.VMEM((TILE, TILE), bf)] * 2
        + [pltpu.VMEM((8, QROWS), jnp.float32), pltpu.VMEM((2, REACH), bf)]
        + [pltpu.VMEM((OT, LANES), bf), pltpu.VMEM((OT, LANES), jnp.int32)]
        + [dma((n + 1,))] * 6 + [dma((15,))] * 2 + [pltpu.SemaphoreType.REGULAR] * 2,
        compiler_params=pltpu.CompilerParams(collective_id=0, has_side_effects=True, vmem_limit_bytes=48 << 20),
        name="slopes",
    )(counts, returns, market, mask)


def per_device(returns, market, mask, counts):
    sizes = (16, 16, 32, 32, 32, 32, 32, 32, 16, 16)
    far = lambda a: pltpu.with_memory_space_constraint(a, pltpu.HBM)
    return slopes(counts, returns, far(market.reshape(OT, LANES)), far(mask.reshape(OT, LANES)), sizes)


def solution(mesh):
    return jax.shard_map(
        per_device,
        mesh=mesh,
        in_specs=(P(None, "span"), P("span"), P("span"), P("span")),
        out_specs=P(None, "span"),
        check_vma=False,
    )
```

```python
import functools

import jax
import jax.numpy as jnp
from jax import lax
from jax.experimental import pallas as pl
from jax.experimental.pallas import tpu as pltpu
from jax.sharding import PartitionSpec as P

WIN = 1024
QROWS = 4096
CAP = 2 * QROWS
REACH = QROWS + WIN
RIDGE = 0.1
LANES = 128
TILE = 256
RT = REACH // LANES
OT = CAP // LANES
TT = WIN // LANES
MESH = pl.DeviceIdType.MESH
ZS, XS, YS = 8, 4, 4


def rolled(load, start, tiles, rows):
    first = lax.shift_right_logical(start, 7)
    r = jnp.bitwise_and(start, LANES - 1)
    turn = jnp.bitwise_and(LANES - r, LANES - 1)
    keep = lax.broadcasted_iota(jnp.int32, (rows, LANES), 1) < LANES - r
    turned = [pltpu.roll(load(first + j), turn, 1) for j in range(tiles + 1)]
    return [jnp.where(keep, turned[j], turned[j + 1]) for j in range(tiles)]


def moved_right(tiles, ticks, count):
    r = jnp.bitwise_and(ticks, LANES - 1)
    turned = [pltpu.roll(tile, r, 1) for tile in tiles]
    low = lax.broadcasted_iota(jnp.int32, tiles[0].shape, 1) < r
    n = len(tiles)
    at = {i: jnp.where(low, turned[max(i - 1, 0)], turned[min(i, n - 1)]) for i in range(n + 1)}
    for bit in (32, 16, 8, 4, 2, 1):
        taken = jnp.bitwise_and(ticks, bit * LANES) != 0
        moved = {}
        for i in range(count):
            if i in at and i - bit in at:
                moved[i] = jnp.where(taken, at[i - bit], at[i])
            elif i in at or i - bit in at:
                moved[i] = at[i] if i in at else at[i - bit]
        at = moved
    return at


def aligned(tiles, far_tiles, excess, edge):
    m = tiles.shape[1]
    parts = rolled(lambda k: tiles[jnp.minimum(jnp.maximum(k, 0), RT + OT - 1)], QROWS - excess, RT, m)
    older = rolled(lambda k: far_tiles[jnp.minimum(jnp.maximum(k, 0), TT - 1)], WIN - jnp.maximum(edge, 0), TT, m)
    lane = lax.broadcasted_iota(jnp.int32, (m, LANES), 1)
    for j in range(TT):
        parts[j] = jnp.where(lane < edge - j * LANES, older[j], parts[j])
    return jnp.concatenate(parts, 1)


def window_sums(a, pre, suf):
    m = a.shape[0]
    tiles, halo = REACH // TILE, WIN // TILE
    stack = jnp.concatenate([a[:, t * TILE : (t + 1) * TILE] for t in range(tiles)], 0)
    head = jnp.dot(stack, pre[...], preferred_element_type=jnp.float32)
    tail = jnp.dot(stack[: (tiles - halo) * m], suf[...], preferred_element_type=jnp.float32)
    whole = [head[t * m : (t + 1) * m, TILE - 1 :] for t in range(tiles)]
    result = []
    for t in range(halo, tiles):
        between = whole[t - 3] + whole[t - 2] + whole[t - 1]
        s = t - halo
        result.append(head[t * m : (t + 1) * m] + tail[s * m : (s + 1) * m] + between)
    return result


def span_kernel(sizes, counts, returns, market_in, mask_in, out, *scratch):
    groups = len(sizes)
    starts = [sum(sizes[:g]) for g in range(groups)]
    n = groups + 1
    it = iter(scratch)
    take = lambda k=n: [next(it) for _ in range(k)]
    ends, send, near, far, tiled, fars = take(), take(), take(), take(), take(), take()
    own = take(groups)
    pairin, zbuf, xbuf, ybuf, ebuf, place = take(6)
    pre, suf, stats, wx, market, mask = take(6)
    own_sem, near_ssem, cross_ssem, near_rsem, far_ssem, far_rsem, cnt_ssem, cnt_rsem, leg_ssem, leg_rsem, present, ready = take(12)
    legs = take(2)

    me = lax.axis_index("span")
    total = ZS * XS * YS * 2
    even = lax.rem(me, 2) == 0
    odd = lax.rem(me, 2) == 1
    last = me == total - 1
    chip = lax.div(me, 2)
    z = lax.rem(chip, ZS)
    x = lax.rem(lax.div(chip, ZS), XS)
    y = lax.div(chip, ZS * XS)

    odd_core = lax.rem(me, 2) == 1

    def core0(yy, xx, zz):
        return ((yy * XS + xx) * ZS + zz) * 2

    def at_z(step):
        return core0(y, x, lax.rem(z + step + ZS, ZS))

    def at_x(step):
        return core0(y, lax.rem(x + step, XS), z)

    def at_y(step):
        return core0(lax.rem(y + step, YS), x, z)

    around = [k for k in range(groups) if sizes[k] == 32][-2:]
    rest = [k for k in range(1, groups) if k not in around]
    order = [0, groups] + around + rest
    done = [groups, 0] + rest[:-2] + around + rest[-2:]
    inner = lax.div(me, 2 * ZS) < XS * YS - 1
    leg = jnp.logical_and(odd_core, jnp.logical_and(inner, jnp.logical_or(z == 1, z == 4)))

    def remote(src, dst, ssem, rsem, target):
        return pltpu.make_async_remote_copy(
            src_ref=src, dst_ref=dst, send_sem=ssem, recv_sem=rsem, device_id=(target,), device_id_type=MESH
        )

    series = [
        pltpu.make_async_copy(market_in, market, own_sem.at[groups]),
        pltpu.make_async_copy(mask_in, mask, own_sem.at[n]),
    ]
    loads = [
        pltpu.make_async_copy(returns.at[pl.ds(starts[g], sizes[g]), :], own[g], own_sem.at[g]) for g in range(groups)
    ]
    loads[0].start()
    for load in series:
        load.start()

    barrier = pltpu.get_barrier_semaphore()

    def hello(target):
        pl.semaphore_signal(barrier, inc=1, device_id=(target,), device_id_type=MESH)

    mine = counts[0]

    @pl.when(even)
    def _():
        hello(me + 1)

        @pl.when(me > 0)
        def _():
            hello(me - 1)

        for step in (1, 2, -1, -2):
            hello(at_z(step))
        for step in (1, 2, 3):
            hello(at_x(step))

            @pl.when(y + step < YS)
            def _(step=step):
                hello(at_y(step))

    @pl.when(jnp.logical_and(even, jnp.logical_and(z == 0, me > 0)))
    def _():
        hello(me - 13)

    @pl.when(leg)
    def _():
        hello(me + 6)

    pairin[...] = jnp.zeros_like(pairin) + mine

    @pl.when(me == 0)
    def _():
        for g in order:
            near[g][...] = jnp.zeros_like(near[g])

    def end_window(g):
        m = ends[g].shape[0]
        if g == groups:
            for load in series:
                load.wait()
            w = mask[...].astype(jnp.float32)
            v = market[...].astype(jnp.float32) * w
            for t in range(OT):
                tiled[g][RT + t] = jnp.concatenate([v[t : t + 1], w[t : t + 1]], 0).astype(jnp.bfloat16)
        else:
            loads[g].wait()
            for t in range(OT):
                tiled[g][RT + t] = own[g][:, t * LANES : (t + 1) * LANES]
        slot = lambda k: tiled[g][jnp.minimum(jnp.maximum(k, RT), RT + OT - 1)]
        for j, value in enumerate(rolled(slot, mine, RT, m)):
            ends[g][:, j * LANES : (j + 1) * LANES] = value

    def cross(g):
        @pl.when(odd)
        def _():
            remote(ends[g], near[g], near_ssem.at[g], near_rsem.at[g], me - 1).wait_recv()
            short = jnp.maximum(REACH - mine, 0)

            @pl.when(jnp.logical_not(last))
            def _():
                m = ends[g].shape[0]
                for first in range(0, m, 16):
                    part = min(m, 16)
                    b = slice(first, first + part)
                    tail = [near[g][b, QROWS + j * LANES : QROWS + (j + 1) * LANES] for j in range(TT)]
                    placed = moved_right(tail, short, RT + TT)
                    lane = lax.broadcasted_iota(jnp.int32, (part, LANES), 1)
                    for j in range(RT):
                        c = slice(j * LANES, (j + 1) * LANES)
                        send[g][b, c] = jnp.where(lane < short - j * LANES, placed[j + TT], ends[g][b, c])
                if g in around:
                    k = around.index(g)

                    @pl.when(z == ZS - 1)
                    def _():
                        remote(send[g], legs[k], cross_ssem.at[g], leg_rsem.at[k], me - 6).start()

                    @pl.when(z < ZS - 1)
                    def _():
                        remote(send[g], near[g], cross_ssem.at[g], near_rsem.at[g], me + 1).start()
                else:
                    remote(send[g], near[g], cross_ssem.at[g], near_rsem.at[g], me + 1).start()

    def to_partner(g):
        @pl.when(even)
        def _():
            remote(ends[g], near[g], near_ssem.at[g], near_rsem.at[g], me + 1).start()

    end_window(order[0])
    for g in order[2:]:
        loads[g].start()
    end_window(order[1])

    @pl.when(odd)
    def _():
        more = jnp.logical_and(inner, jnp.logical_or(jnp.logical_or(z == 1, z == 4), z == 7))
        pl.semaphore_wait(barrier, 2 - jnp.where(last, 1, 0) + jnp.where(more, 1, 0))
        pl.semaphore_signal(present, inc=1, device_id=(me - 1,), device_id_type=MESH)
        remote(pairin, zbuf.at[0], cnt_ssem.at[0], cnt_rsem.at[0], me - 1).start()

    @pl.when(even)
    def _():
        pl.semaphore_wait(present, 1)

    to_partner(order[0])
    to_partner(order[1])
    for i in range(2, n):
        end_window(order[i])
        to_partner(order[i])
        cross(order[i - 2])
    cross(order[n - 2])
    cross(order[n - 1])

    def onward(k, start):
        @pl.when(z == 4)
        def _():
            start(remote(legs[k], legs[k], leg_ssem.at[k], leg_rsem.at[k], me - 6))

        @pl.when(z == 1)
        def _():
            start(remote(legs[k], near[around[k]], leg_ssem.at[k], near_rsem.at[around[k]], me + 13))

    @pl.when(leg)
    def _():
        for k in range(len(around)):
            remote(legs[k], legs[k], leg_ssem.at[k], leg_rsem.at[k], me + 6).wait_recv()
            onward(k, lambda copy: copy.start())

    q = lax.broadcasted_iota(jnp.int32, (TILE, TILE), 0)
    p = lax.broadcasted_iota(jnp.int32, (TILE, TILE), 1)
    pre[...] = jnp.where(q <= p, 1.0, 0.0).astype(jnp.bfloat16)
    suf[...] = jnp.where(q > p, 1.0, 0.0).astype(jnp.bfloat16)

    @pl.when(even)
    def _():
        def arrival(dst, k):
            return remote(dst, dst, cnt_ssem.at[k], cnt_rsem.at[k], me + 1)

        sends = []

        def push(ref, target, k):
            copy = remote(ref, ref, cnt_ssem.at[k], cnt_rsem.at[k], target)
            copy.start()
            sends.append(copy)

        pl.semaphore_wait(barrier, 7 + y)
        for step in (1, 2, 3):
            @pl.when(y >= step)
            def _(step=step):
                pl.semaphore_signal(ready, inc=1, device_id=(core0(y - step, x, z),), device_id_type=MESH)

        arrival(zbuf.at[0], 0).wait_recv()
        zbuf[z + 1] = zbuf[0] + mine
        for k, step in ((1, 1), (2, 2), (3, -1), (4, -2)):
            push(zbuf.at[z + 1], at_z(step), k)
        back1, back2 = lax.rem(z + ZS - 1, ZS), lax.rem(z + ZS - 2, ZS)
        ahead1, ahead2 = lax.rem(z + 1, ZS), lax.rem(z + 2, ZS)
        back3, back4, ahead3 = lax.rem(z + ZS - 3, ZS), lax.rem(z + ZS - 4, ZS), lax.rem(z + 3, ZS)
        for k, slot in ((1, back1), (2, back2), (3, ahead1), (4, ahead2)):
            arrival(zbuf.at[slot + 1], k).wait_recv()
        push(zbuf.at[back2 + 1], at_z(1), 5)
        push(zbuf.at[back2 + 1], at_z(2), 6)
        push(zbuf.at[ahead2 + 1], at_z(-1), 7)
        for k, slot in ((5, back3), (6, back4), (7, ahead3)):
            arrival(zbuf.at[slot + 1], k).wait_recv()
        column = zbuf[1]
        below = jnp.where(z > 0, zbuf[1], 0)
        for i in range(1, ZS):
            column = column + zbuf[i + 1]
            below = below + jnp.where(z > i, zbuf[i + 1], 0)
        xbuf[x] = column
        for step in (1, 2, 3):
            push(xbuf.at[x], at_x(step), 7 + step)
        for step in (1, 2, 3):
            arrival(xbuf.at[lax.rem(x + XS - step, XS)], 7 + step).wait_recv()
        plane = xbuf[0]
        below = below + jnp.where(x > 0, xbuf[0], 0)
        for i in range(1, XS):
            plane = plane + xbuf[i]
            below = below + jnp.where(x > i, xbuf[i], 0)
        ybuf[y] = plane
        @pl.when(y < YS - 1)
        def _():
            pl.semaphore_wait(ready, YS - 1 - y)

        for step in (1, 2, 3):
            up = remote(ybuf.at[y], ybuf.at[y], cnt_ssem.at[10 + step], cnt_rsem.at[10 + step], at_y(step))
            pl.when(y + step < YS)(up.start)
        for step in (1, 2, 3):
            @pl.when(y >= step)
            def _(step=step):
                arrival(ybuf.at[y - step], 10 + step).wait_recv()
        for i in range(YS):
            below = below + jnp.where(y > i, ybuf[i], 0)
        ebuf[0] = below - me * QROWS
        ebuf[1] = below + mine - (me + 1) * QROWS
        copy = remote(ebuf.at[pl.ds(0, 2)], ebuf.at[pl.ds(2, 2)], cnt_ssem.at[14], cnt_rsem.at[14], me + 1)
        copy.start()
        sends.append(copy)
        place[0] = ebuf[0]
        place[1] = jnp.full_like(ebuf[0], -1)
        for copy in sends:
            copy.wait_send()
        for step in (1, 2, 3):
            up = remote(ybuf.at[y], ybuf.at[y], cnt_ssem.at[10 + step], cnt_rsem.at[10 + step], at_y(step))
            pl.when(y + step < YS)(up.wait_send)

    @pl.when(odd)
    def _():
        remote(ebuf.at[pl.ds(0, 2)], ebuf.at[pl.ds(2, 2)], cnt_ssem.at[14], cnt_rsem.at[14], me - 1).wait_recv()
        place[0] = ebuf[3]
        place[1] = ebuf[2] - (QROWS - WIN)

    excess = jnp.max(place[0])
    edge = jnp.max(place[1])
    for g in done:
        piece = near[g].at[:, pl.ds(QROWS, WIN)]

        @pl.when(even)
        def _():
            @pl.when(me > 0)
            def _():
                remote(send[g], near[g], cross_ssem.at[g], near_rsem.at[g], me + 1).wait_recv()

            remote(piece, far[g], far_ssem.at[g], far_rsem.at[g], me + 1).start()

        for t in range(RT):
            tiled[g][t] = near[g][:, t * LANES : (t + 1) * LANES]

        @pl.when(odd)
        def _():
            remote(piece, far[g], far_ssem.at[g], far_rsem.at[g], me - 1).wait_recv()
            for t in range(TT):
                fars[g][t] = far[g][:, t * LANES : (t + 1) * LANES]

        ticks = aligned(tiled[g], fars[g], excess, edge)
        if g == groups:
            wx[...] = ticks
            xf = ticks[0:1, :].astype(jnp.float32)
            wf = ticks[1:2, :].astype(jnp.float32)
            row = lax.broadcasted_iota(jnp.int32, (16, REACH), 0)
            a = jnp.where(row == 0, wf, jnp.where(row == 1, xf, xf * xf)).astype(jnp.bfloat16)
            for i, s in enumerate(window_sums(a, pre, suf)):
                c = slice(i * TILE, (i + 1) * TILE)
                sw, sx, sxx = s[0:1], s[1:2], s[2:3]
                stats[0:1, c] = sw
                stats[1:2, c] = sx
                stats[2:3, c] = 1.0 / (sw * sxx - sx * sx + RIDGE * WIN * WIN)
        else:
            m = sizes[g]
            yv = ticks * wx[1:2, :]
            crossed = (wx[0:1, :].astype(jnp.float32) * yv.astype(jnp.float32)).astype(jnp.bfloat16)
            for i, s in enumerate(window_sums(jnp.concatenate([crossed, yv], 0), pre, suf)):
                c = slice(i * TILE, (i + 1) * TILE)
                value = (stats[0:1, c] * s[:m] - stats[1:2, c] * s[m:]) * stats[2:3, c]
                out[starts[g] : starts[g] + m, c] = value

    @pl.when(even)
    def _():
        for g in order:
            remote(ends[g], near[g], near_ssem.at[g], near_rsem.at[g], me + 1).wait_send()
            remote(near[g].at[:, pl.ds(QROWS, WIN)], far[g], far_ssem.at[g], far_rsem.at[g], me + 1).wait_send()

    @pl.when(odd)
    def _():
        remote(pairin, zbuf.at[0], cnt_ssem.at[0], cnt_rsem.at[0], me - 1).wait_send()

        @pl.when(jnp.logical_not(last))
        def _():
            for g in order:
                remote(send[g], near[g], cross_ssem.at[g], near_rsem.at[g], me + 1).wait_send()

        @pl.when(leg)
        def _():
            for k in range(len(around)):
                onward(k, lambda copy: copy.wait_send())


def slopes(counts, returns, market, mask, sizes):
    stocks = returns.shape[0]
    bf = jnp.bfloat16

    def per(shape):
        return [pltpu.VMEM(shape(m), bf) for m in list(sizes) + [2]]

    flat = lambda length: per(lambda m: (m, length))
    split = lambda count: per(lambda m: (count, m, LANES))
    n = len(sizes) + 1
    dma = pltpu.SemaphoreType.DMA
    row = lambda k: pltpu.VMEM((k, 1, LANES), jnp.int32)
    vmem = pl.BlockSpec(memory_space=pltpu.VMEM)
    return pl.pallas_call(
        functools.partial(span_kernel, sizes),
        out_shape=jax.ShapeDtypeStruct((stocks, QROWS), jnp.float32),
        in_specs=[pl.BlockSpec(memory_space=pltpu.SMEM)] + [pl.BlockSpec(memory_space=pltpu.HBM)] * 3,
        out_specs=vmem,
        scratch_shapes=flat(REACH) + flat(REACH) + flat(REACH) + flat(WIN) + split(RT + OT) + split(TT)
        + flat(CAP)[:-1]
        + [pltpu.VMEM((1, LANES), jnp.int32), row(ZS + 1), row(XS), row(YS), row(4), row(2)]
        + [pltpu.VMEM((TILE, TILE), bf)] * 2
        + [pltpu.VMEM((8, QROWS), jnp.float32), pltpu.VMEM((2, REACH), bf)]
        + [pltpu.VMEM((OT, LANES), bf), pltpu.VMEM((OT, LANES), jnp.int32)]
        + [dma((n + 1,))] * 6 + [dma((15,))] * 2 + [dma((2,))] * 2 + [pltpu.SemaphoreType.REGULAR] * 2
        + [pltpu.VMEM((32, REACH), bf)] * 2,
        compiler_params=pltpu.CompilerParams(collective_id=0, has_side_effects=True, vmem_limit_bytes=48 << 20),
        name="slopes",
    )(counts, returns, market, mask)


def per_device(returns, market, mask, counts):
    sizes = (16, 16, 32, 32, 32, 32, 32, 32, 16, 16)
    far = lambda a: pltpu.with_memory_space_constraint(a, pltpu.HBM)
    return slopes(counts, returns, far(market.reshape(OT, LANES)), far(mask.reshape(OT, LANES)), sizes)


def solution(mesh):
    return jax.shard_map(
        per_device,
        mesh=mesh,
        in_specs=(P(None, "span"), P("span"), P("span"), P("span")),
        out_specs=P(None, "span"),
        check_vma=False,
    )
```

```python
import functools

import jax
import jax.numpy as jnp
from jax import lax
from jax.experimental import pallas as pl
from jax.experimental.pallas import tpu as pltpu
from jax.sharding import PartitionSpec as P

WIN = 1024
QROWS = 4096
CAP = 2 * QROWS
REACH = QROWS + WIN
RIDGE = 0.1
LANES = 128
TILE = 256
RT = REACH // LANES
OT = CAP // LANES
TT = WIN // LANES
MESH = pl.DeviceIdType.MESH
ZS, XS, YS = 8, 4, 4


def rolled(load, start, tiles, rows):
    first = lax.shift_right_logical(start, 7)
    r = jnp.bitwise_and(start, LANES - 1)
    turn = jnp.bitwise_and(LANES - r, LANES - 1)
    keep = lax.broadcasted_iota(jnp.int32, (rows, LANES), 1) < LANES - r
    turned = [pltpu.roll(load(first + j), turn, 1) for j in range(tiles + 1)]
    return [jnp.where(keep, turned[j], turned[j + 1]) for j in range(tiles)]


def moved_right(tiles, ticks, count):
    r = jnp.bitwise_and(ticks, LANES - 1)
    turned = [pltpu.roll(tile, r, 1) for tile in tiles]
    low = lax.broadcasted_iota(jnp.int32, tiles[0].shape, 1) < r
    n = len(tiles)
    at = {i: jnp.where(low, turned[max(i - 1, 0)], turned[min(i, n - 1)]) for i in range(n + 1)}
    for bit in (32, 16, 8, 4, 2, 1):
        taken = jnp.bitwise_and(ticks, bit * LANES) != 0
        moved = {}
        for i in range(count):
            if i in at and i - bit in at:
                moved[i] = jnp.where(taken, at[i - bit], at[i])
            elif i in at or i - bit in at:
                moved[i] = at[i] if i in at else at[i - bit]
        at = moved
    return at


def aligned(tiles, far_tiles, excess, edge):
    m = tiles.shape[1]
    parts = rolled(lambda k: tiles[jnp.minimum(jnp.maximum(k, 0), RT + OT - 1)], QROWS - excess, RT, m)
    older = rolled(lambda k: far_tiles[jnp.minimum(jnp.maximum(k, 0), TT - 1)], WIN - jnp.maximum(edge, 0), TT, m)
    lane = lax.broadcasted_iota(jnp.int32, (m, LANES), 1)
    for j in range(TT):
        parts[j] = jnp.where(lane < edge - j * LANES, older[j], parts[j])
    return jnp.concatenate(parts, 1)


def window_sums(a, pre, suf):
    m = a.shape[0]
    tiles, halo = REACH // TILE, WIN // TILE
    stack = jnp.concatenate([a[:, t * TILE : (t + 1) * TILE] for t in range(tiles)], 0)
    head = jnp.dot(stack, pre[...], preferred_element_type=jnp.float32)
    tail = jnp.dot(stack[: (tiles - halo) * m], suf[...], preferred_element_type=jnp.float32)
    whole = [head[t * m : (t + 1) * m, TILE - 1 :] for t in range(tiles)]
    result = []
    for t in range(halo, tiles):
        between = whole[t - 3] + whole[t - 2] + whole[t - 1]
        s = t - halo
        result.append(head[t * m : (t + 1) * m] + tail[s * m : (s + 1) * m] + between)
    return result


def span_kernel(sizes, counts, returns, market_in, mask_in, out, *scratch):
    groups = len(sizes)
    starts = [sum(sizes[:g]) for g in range(groups)]
    n = groups + 1
    it = iter(scratch)
    take = lambda k=n: [next(it) for _ in range(k)]
    ends, send, near, far, tiled, fars = take(), take(), take(), take(), take(), take()
    own = take(groups)
    pairin, zbuf, xbuf, ybuf, ebuf, place = take(6)
    pre, suf, stats, wx, market, mask = take(6)
    own_sem, near_ssem, cross_ssem, near_rsem, far_ssem, far_rsem, cnt_ssem, cnt_rsem, leg_ssem, leg_rsem, present, ready = take(12)
    legs = take(2)

    me = lax.axis_index("span")
    total = ZS * XS * YS * 2
    even = lax.rem(me, 2) == 0
    odd = lax.rem(me, 2) == 1
    last = me == total - 1
    chip = lax.div(me, 2)
    z = lax.rem(chip, ZS)
    x = lax.rem(lax.div(chip, ZS), XS)
    y = lax.div(chip, ZS * XS)

    odd_core = lax.rem(me, 2) == 1

    def core0(yy, xx, zz):
        return ((yy * XS + xx) * ZS + zz) * 2

    def at_z(step):
        return core0(y, x, lax.rem(z + step + ZS, ZS))

    def at_x(step):
        return core0(y, lax.rem(x + step, XS), z)

    def at_y(step):
        return core0(lax.rem(y + step, YS), x, z)

    around = [7, 1]
    rest = [k for k in range(1, groups) if k not in around]
    order = [0, groups] + around + rest
    done = [groups, 0] + rest[:-2] + around + rest[-2:]
    column = lax.div(me, 2 * ZS)
    inner = column < XS * YS - 1
    leg_a = jnp.logical_and(odd_core, jnp.logical_and(inner, z == 4))
    leg_b = jnp.logical_and(odd_core, jnp.logical_and(column > 0, z == 1))
    first_leg = jnp.logical_and(odd_core, jnp.logical_and(inner, z == 7))

    def remote(src, dst, ssem, rsem, target):
        return pltpu.make_async_remote_copy(
            src_ref=src, dst_ref=dst, send_sem=ssem, recv_sem=rsem, device_id=(target,), device_id_type=MESH
        )

    series = [
        pltpu.make_async_copy(market_in, market, own_sem.at[groups]),
        pltpu.make_async_copy(mask_in, mask, own_sem.at[n]),
    ]
    loads = [
        pltpu.make_async_copy(returns.at[pl.ds(starts[g], sizes[g]), :], own[g], own_sem.at[g]) for g in range(groups)
    ]
    loads[0].start()
    for load in series:
        load.start()

    barrier = pltpu.get_barrier_semaphore()

    def hello(target):
        pl.semaphore_signal(barrier, inc=1, device_id=(target,), device_id_type=MESH)

    mine = counts[0]

    @pl.when(even)
    def _():
        hello(me + 1)

        @pl.when(me > 0)
        def _():
            hello(me - 1)

        for step in (1, 2, -1, -2):
            hello(at_z(step))
        for step in (1, 2, 3):
            hello(at_x(step))

            @pl.when(y + step < YS)
            def _(step=step):
                hello(at_y(step))

    @pl.when(jnp.logical_and(even, jnp.logical_and(z == 0, me > 0)))
    def _():
        hello(me + 3)

    @pl.when(leg_b)
    def _():
        hello(me - 10)

    @pl.when(leg_a)
    def _():
        hello(me + 6)

    pairin[...] = jnp.zeros_like(pairin) + mine

    @pl.when(me == 0)
    def _():
        for g in order:
            near[g][...] = jnp.zeros_like(near[g])

    def end_window(g):
        m = ends[g].shape[0]
        if g == groups:
            for load in series:
                load.wait()
            w = mask[...].astype(jnp.float32)
            v = market[...].astype(jnp.float32) * w
            for t in range(OT):
                tiled[g][RT + t] = jnp.concatenate([v[t : t + 1], w[t : t + 1]], 0).astype(jnp.bfloat16)
        else:
            loads[g].wait()
            for t in range(OT):
                tiled[g][RT + t] = own[g][:, t * LANES : (t + 1) * LANES]
        slot = lambda k: tiled[g][jnp.minimum(jnp.maximum(k, RT), RT + OT - 1)]
        for j, value in enumerate(rolled(slot, mine, RT, m)):
            ends[g][:, j * LANES : (j + 1) * LANES] = value

    def cross(g):
        @pl.when(odd)
        def _():
            remote(ends[g], near[g], near_ssem.at[g], near_rsem.at[g], me - 1).wait_recv()
            short = jnp.maximum(REACH - mine, 0)

            @pl.when(jnp.logical_not(last))
            def _():
                m = ends[g].shape[0]
                for first in range(0, m, 16):
                    part = min(m, 16)
                    b = slice(first, first + part)
                    tail = [near[g][b, QROWS + j * LANES : QROWS + (j + 1) * LANES] for j in range(TT)]
                    placed = moved_right(tail, short, RT + TT)
                    lane = lax.broadcasted_iota(jnp.int32, (part, LANES), 1)
                    for j in range(RT):
                        c = slice(j * LANES, (j + 1) * LANES)
                        send[g][b, c] = jnp.where(lane < short - j * LANES, placed[j + TT], ends[g][b, c])
                if g in around:
                    k = around.index(g)

                    @pl.when(z == ZS - 1)
                    def _():
                        remote(send[g], legs[k], cross_ssem.at[g], leg_rsem.at[k], me - 6).start()

                    @pl.when(z < ZS - 1)
                    def _():
                        remote(send[g], near[g], cross_ssem.at[g], near_rsem.at[g], me + 1).start()
                else:
                    remote(send[g], near[g], cross_ssem.at[g], near_rsem.at[g], me + 1).start()

    def to_partner(g):
        @pl.when(even)
        def _():
            remote(ends[g], near[g], near_ssem.at[g], near_rsem.at[g], me + 1).start()

    for g in order[2:]:
        loads[g].start()
    end_window(order[0])

    @pl.when(odd)
    def _():
        more = jnp.logical_or(jnp.logical_or(leg_a, leg_b), first_leg)
        pl.semaphore_wait(barrier, 2 - jnp.where(last, 1, 0) + jnp.where(more, 1, 0))
        pl.semaphore_signal(present, inc=1, device_id=(me - 1,), device_id_type=MESH)
        remote(pairin, zbuf.at[0], cnt_ssem.at[0], cnt_rsem.at[0], me - 1).start()

    @pl.when(even)
    def _():
        pl.semaphore_wait(present, 1)

    to_partner(order[0])
    end_window(order[1])
    to_partner(order[1])
    cross(order[0])
    for i in range(2, n):
        end_window(order[i])
        to_partner(order[i])
        cross(order[i - 1])
    cross(order[n - 1])

    def onward_a(k):
        return remote(legs[k], legs[k], leg_ssem.at[k], leg_rsem.at[k], me + 10)

    def onward_b(k):
        return remote(legs[k], near[around[k]], leg_ssem.at[k], near_rsem.at[around[k]], me - 3)

    for on, onward in ((leg_a, onward_a), (leg_b, onward_b)):
        @pl.when(on)
        def _(onward=onward):
            for k in range(len(around)):
                onward_a(k).wait_recv()
                onward(k).start()

    q = lax.broadcasted_iota(jnp.int32, (TILE, TILE), 0)
    p = lax.broadcasted_iota(jnp.int32, (TILE, TILE), 1)
    pre[...] = jnp.where(q <= p, 1.0, 0.0).astype(jnp.bfloat16)
    suf[...] = jnp.where(q > p, 1.0, 0.0).astype(jnp.bfloat16)

    @pl.when(even)
    def _():
        def arrival(dst, k):
            return remote(dst, dst, cnt_ssem.at[k], cnt_rsem.at[k], me + 1)

        sends = []

        def push(ref, target, k):
            copy = remote(ref, ref, cnt_ssem.at[k], cnt_rsem.at[k], target)
            copy.start()
            sends.append(copy)

        pl.semaphore_wait(barrier, 7 + y)
        for step in (1, 2, 3):
            @pl.when(y >= step)
            def _(step=step):
                pl.semaphore_signal(ready, inc=1, device_id=(core0(y - step, x, z),), device_id_type=MESH)

        arrival(zbuf.at[0], 0).wait_recv()
        zbuf[z + 1] = zbuf[0] + mine
        for k, step in ((1, 1), (2, 2), (3, -1), (4, -2)):
            push(zbuf.at[z + 1], at_z(step), k)
        back1, back2 = lax.rem(z + ZS - 1, ZS), lax.rem(z + ZS - 2, ZS)
        ahead1, ahead2 = lax.rem(z + 1, ZS), lax.rem(z + 2, ZS)
        back3, back4, ahead3 = lax.rem(z + ZS - 3, ZS), lax.rem(z + ZS - 4, ZS), lax.rem(z + 3, ZS)
        for k, slot in ((1, back1), (2, back2), (3, ahead1), (4, ahead2)):
            arrival(zbuf.at[slot + 1], k).wait_recv()
        push(zbuf.at[back2 + 1], at_z(1), 5)
        push(zbuf.at[back2 + 1], at_z(2), 6)
        push(zbuf.at[ahead2 + 1], at_z(-1), 7)
        for k, slot in ((5, back3), (6, back4), (7, ahead3)):
            arrival(zbuf.at[slot + 1], k).wait_recv()
        column = zbuf[1]
        below = jnp.where(z > 0, zbuf[1], 0)
        for i in range(1, ZS):
            column = column + zbuf[i + 1]
            below = below + jnp.where(z > i, zbuf[i + 1], 0)
        xbuf[x] = column
        for step in (1, 2, 3):
            push(xbuf.at[x], at_x(step), 7 + step)
        for step in (1, 2, 3):
            arrival(xbuf.at[lax.rem(x + XS - step, XS)], 7 + step).wait_recv()
        plane = xbuf[0]
        below = below + jnp.where(x > 0, xbuf[0], 0)
        for i in range(1, XS):
            plane = plane + xbuf[i]
            below = below + jnp.where(x > i, xbuf[i], 0)
        ybuf[y] = plane
        @pl.when(y < YS - 1)
        def _():
            pl.semaphore_wait(ready, YS - 1 - y)

        for step in (1, 2, 3):
            up = remote(ybuf.at[y], ybuf.at[y], cnt_ssem.at[10 + step], cnt_rsem.at[10 + step], at_y(step))
            pl.when(y + step < YS)(up.start)
        for step in (1, 2, 3):
            @pl.when(y >= step)
            def _(step=step):
                arrival(ybuf.at[y - step], 10 + step).wait_recv()
        for i in range(YS):
            below = below + jnp.where(y > i, ybuf[i], 0)
        ebuf[0] = below - me * QROWS
        ebuf[1] = below + mine - (me + 1) * QROWS
        copy = remote(ebuf.at[pl.ds(0, 2)], ebuf.at[pl.ds(2, 2)], cnt_ssem.at[14], cnt_rsem.at[14], me + 1)
        copy.start()
        sends.append(copy)
        place[0] = ebuf[0]
        place[1] = jnp.full_like(ebuf[0], -1)
        for copy in sends:
            copy.wait_send()
        for step in (1, 2, 3):
            up = remote(ybuf.at[y], ybuf.at[y], cnt_ssem.at[10 + step], cnt_rsem.at[10 + step], at_y(step))
            pl.when(y + step < YS)(up.wait_send)

    @pl.when(odd)
    def _():
        remote(ebuf.at[pl.ds(0, 2)], ebuf.at[pl.ds(2, 2)], cnt_ssem.at[14], cnt_rsem.at[14], me - 1).wait_recv()
        place[0] = ebuf[3]
        place[1] = ebuf[2] - (QROWS - WIN)

    excess = jnp.max(place[0])
    edge = jnp.max(place[1])
    for g in done:
        piece = near[g].at[:, pl.ds(QROWS, WIN)]

        @pl.when(even)
        def _():
            @pl.when(me > 0)
            def _():
                remote(send[g], near[g], cross_ssem.at[g], near_rsem.at[g], me + 1).wait_recv()

            remote(piece, far[g], far_ssem.at[g], far_rsem.at[g], me + 1).start()

        for t in range(RT):
            tiled[g][t] = near[g][:, t * LANES : (t + 1) * LANES]

        @pl.when(odd)
        def _():
            remote(piece, far[g], far_ssem.at[g], far_rsem.at[g], me - 1).wait_recv()
            for t in range(TT):
                fars[g][t] = far[g][:, t * LANES : (t + 1) * LANES]

        ticks = aligned(tiled[g], fars[g], excess, edge)
        if g == groups:
            wx[...] = ticks
            xf = ticks[0:1, :].astype(jnp.float32)
            wf = ticks[1:2, :].astype(jnp.float32)
            row = lax.broadcasted_iota(jnp.int32, (16, REACH), 0)
            a = jnp.where(row == 0, wf, jnp.where(row == 1, xf, xf * xf)).astype(jnp.bfloat16)
            for i, s in enumerate(window_sums(a, pre, suf)):
                c = slice(i * TILE, (i + 1) * TILE)
                sw, sx, sxx = s[0:1], s[1:2], s[2:3]
                stats[0:1, c] = sw
                stats[1:2, c] = sx
                stats[2:3, c] = 1.0 / (sw * sxx - sx * sx + RIDGE * WIN * WIN)
        else:
            m = sizes[g]
            yv = ticks * wx[1:2, :]
            crossed = (wx[0:1, :].astype(jnp.float32) * yv.astype(jnp.float32)).astype(jnp.bfloat16)
            for i, s in enumerate(window_sums(jnp.concatenate([crossed, yv], 0), pre, suf)):
                c = slice(i * TILE, (i + 1) * TILE)
                value = (stats[0:1, c] * s[:m] - stats[1:2, c] * s[m:]) * stats[2:3, c]
                out[starts[g] : starts[g] + m, c] = value

    @pl.when(even)
    def _():
        for g in order:
            remote(ends[g], near[g], near_ssem.at[g], near_rsem.at[g], me + 1).wait_send()
            remote(near[g].at[:, pl.ds(QROWS, WIN)], far[g], far_ssem.at[g], far_rsem.at[g], me + 1).wait_send()

    @pl.when(odd)
    def _():
        remote(pairin, zbuf.at[0], cnt_ssem.at[0], cnt_rsem.at[0], me - 1).wait_send()

        @pl.when(jnp.logical_not(last))
        def _():
            for g in order:
                remote(send[g], near[g], cross_ssem.at[g], near_rsem.at[g], me + 1).wait_send()

        for on, onward in ((leg_a, onward_a), (leg_b, onward_b)):
            @pl.when(on)
            def _(onward=onward):
                for k in range(len(around)):
                    onward(k).wait_send()


def slopes(counts, returns, market, mask, sizes):
    stocks = returns.shape[0]
    bf = jnp.bfloat16

    def per(shape):
        return [pltpu.VMEM(shape(m), bf) for m in list(sizes) + [2]]

    flat = lambda length: per(lambda m: (m, length))
    split = lambda count: per(lambda m: (count, m, LANES))
    n = len(sizes) + 1
    dma = pltpu.SemaphoreType.DMA
    row = lambda k: pltpu.VMEM((k, 1, LANES), jnp.int32)
    vmem = pl.BlockSpec(memory_space=pltpu.VMEM)
    return pl.pallas_call(
        functools.partial(span_kernel, sizes),
        out_shape=jax.ShapeDtypeStruct((stocks, QROWS), jnp.float32),
        in_specs=[pl.BlockSpec(memory_space=pltpu.SMEM)] + [pl.BlockSpec(memory_space=pltpu.HBM)] * 3,
        out_specs=vmem,
        scratch_shapes=flat(REACH) + flat(REACH) + flat(REACH) + flat(WIN) + split(RT + OT) + split(TT)
        + flat(CAP)[:-1]
        + [pltpu.VMEM((1, LANES), jnp.int32), row(ZS + 1), row(XS), row(YS), row(4), row(2)]
        + [pltpu.VMEM((TILE, TILE), bf)] * 2
        + [pltpu.VMEM((8, QROWS), jnp.float32), pltpu.VMEM((2, REACH), bf)]
        + [pltpu.VMEM((OT, LANES), bf), pltpu.VMEM((OT, LANES), jnp.int32)]
        + [dma((n + 1,))] * 6 + [dma((15,))] * 2 + [dma((2,))] * 2 + [pltpu.SemaphoreType.REGULAR] * 2
        + [pltpu.VMEM((sizes[k], REACH), bf) for k in (7, 1)],
        compiler_params=pltpu.CompilerParams(collective_id=0, has_side_effects=True, vmem_limit_bytes=48 << 20),
        name="slopes",
    )(counts, returns, market, mask)


def per_device(returns, market, mask, counts):
    sizes = (16, 16, 32, 32, 32, 32, 32, 32, 16, 16)
    far = lambda a: pltpu.with_memory_space_constraint(a, pltpu.HBM)
    return slopes(counts, returns, far(market.reshape(OT, LANES)), far(mask.reshape(OT, LANES)), sizes)


def solution(mesh):
    return jax.shard_map(
        per_device,
        mesh=mesh,
        in_specs=(P(None, "span"), P("span"), P("span"), P("span")),
        out_specs=P(None, "span"),
        check_vma=False,
    )
```

```python
import functools

import jax
import jax.numpy as jnp
from jax import lax
from jax.experimental import pallas as pl
from jax.experimental.pallas import tpu as pltpu
from jax.sharding import PartitionSpec as P

WIN = 1024
QROWS = 4096
CAP = 2 * QROWS
REACH = QROWS + WIN
RIDGE = 0.1
LANES = 128
TILE = 256
RT = REACH // LANES
OT = CAP // LANES
TT = WIN // LANES
MESH = pl.DeviceIdType.MESH
ZS, XS, YS = 8, 4, 4


def rolled(load, start, tiles, rows):
    first = lax.shift_right_logical(start, 7)
    r = jnp.bitwise_and(start, LANES - 1)
    turn = jnp.bitwise_and(LANES - r, LANES - 1)
    keep = lax.broadcasted_iota(jnp.int32, (rows, LANES), 1) < LANES - r
    turned = [pltpu.roll(load(first + j), turn, 1) for j in range(tiles + 1)]
    return [jnp.where(keep, turned[j], turned[j + 1]) for j in range(tiles)]


def moved_right(tiles, ticks, count):
    r = jnp.bitwise_and(ticks, LANES - 1)
    turned = [pltpu.roll(tile, r, 1) for tile in tiles]
    low = lax.broadcasted_iota(jnp.int32, tiles[0].shape, 1) < r
    n = len(tiles)
    at = {i: jnp.where(low, turned[max(i - 1, 0)], turned[min(i, n - 1)]) for i in range(n + 1)}
    for bit in (32, 16, 8, 4, 2, 1):
        taken = jnp.bitwise_and(ticks, bit * LANES) != 0
        moved = {}
        for i in range(count):
            if i in at and i - bit in at:
                moved[i] = jnp.where(taken, at[i - bit], at[i])
            elif i in at or i - bit in at:
                moved[i] = at[i] if i in at else at[i - bit]
        at = moved
    return at


def aligned(tiles, far_tiles, excess, edge):
    m = tiles.shape[1]
    parts = rolled(lambda k: tiles[jnp.minimum(jnp.maximum(k, 0), RT + OT - 1)], QROWS - excess, RT, m)
    older = rolled(lambda k: far_tiles[jnp.minimum(jnp.maximum(k, 0), TT - 1)], WIN - jnp.maximum(edge, 0), TT, m)
    lane = lax.broadcasted_iota(jnp.int32, (m, LANES), 1)
    for j in range(TT):
        parts[j] = jnp.where(lane < edge - j * LANES, older[j], parts[j])
    return jnp.concatenate(parts, 1)


def window_sums(a, pre, suf):
    m = a.shape[0]
    tiles, halo = REACH // TILE, WIN // TILE
    stack = jnp.concatenate([a[:, t * TILE : (t + 1) * TILE] for t in range(tiles)], 0)
    head = jnp.dot(stack, pre[...], preferred_element_type=jnp.float32)
    tail = jnp.dot(stack[: (tiles - halo) * m], suf[...], preferred_element_type=jnp.float32)
    whole = [head[t * m : (t + 1) * m, TILE - 1 :] for t in range(tiles)]
    result = []
    for t in range(halo, tiles):
        between = whole[t - 3] + whole[t - 2] + whole[t - 1]
        s = t - halo
        result.append(head[t * m : (t + 1) * m] + tail[s * m : (s + 1) * m] + between)
    return result


def span_kernel(sizes, counts, returns, market_in, mask_in, out, *scratch):
    groups = len(sizes)
    starts = [sum(sizes[:g]) for g in range(groups)]
    n = groups + 1
    it = iter(scratch)
    take = lambda k=n: [next(it) for _ in range(k)]
    ends, send, near, far, tiled, fars = take(), take(), take(), take(), take(), take()
    own = take(groups)
    pairin, zbuf, xbuf, ybuf, ebuf, place = take(6)
    pre, suf, stats, wx, market, mask = take(6)
    own_sem, near_ssem, cross_ssem, near_rsem, far_ssem, far_rsem, cnt_ssem, cnt_rsem, leg_ssem, leg_rsem, present, ready = take(12)
    legs = take(2)

    me = lax.axis_index("span")
    total = ZS * XS * YS * 2
    even = lax.rem(me, 2) == 0
    odd = lax.rem(me, 2) == 1
    last = me == total - 1
    chip = lax.div(me, 2)
    z = lax.rem(chip, ZS)
    x = lax.rem(lax.div(chip, ZS), XS)
    y = lax.div(chip, ZS * XS)

    odd_core = lax.rem(me, 2) == 1

    def core0(yy, xx, zz):
        return ((yy * XS + xx) * ZS + zz) * 2

    def at_z(step):
        return core0(y, x, lax.rem(z + step + ZS, ZS))

    def at_x(step):
        return core0(y, lax.rem(x + step, XS), z)

    def at_y(step):
        return core0(lax.rem(y + step, YS), x, z)

    around = [7, 6]
    rest = [k for k in range(1, groups) if k not in around]
    order = [0, groups] + around + rest
    done = [groups, 0] + rest[:-2] + around + rest[-2:]
    column = lax.div(me, 2 * ZS)
    inner = column < XS * YS - 1
    leg_a = jnp.logical_and(odd_core, jnp.logical_and(inner, z == 4))
    leg_b = jnp.logical_and(odd_core, jnp.logical_and(column > 0, z == 1))
    first_leg = jnp.logical_and(odd_core, jnp.logical_and(inner, z == 7))

    def remote(src, dst, ssem, rsem, target):
        return pltpu.make_async_remote_copy(
            src_ref=src, dst_ref=dst, send_sem=ssem, recv_sem=rsem, device_id=(target,), device_id_type=MESH
        )

    series = [
        pltpu.make_async_copy(market_in, market, own_sem.at[groups]),
        pltpu.make_async_copy(mask_in, mask, own_sem.at[n]),
    ]
    loads = [
        pltpu.make_async_copy(returns.at[pl.ds(starts[g], sizes[g]), :], own[g], own_sem.at[g]) for g in range(groups)
    ]
    loads[0].start()
    for load in series:
        load.start()

    barrier = pltpu.get_barrier_semaphore()

    def hello(target):
        pl.semaphore_signal(barrier, inc=1, device_id=(target,), device_id_type=MESH)

    mine = counts[0]

    @pl.when(even)
    def _():
        hello(me + 1)

        @pl.when(me > 0)
        def _():
            hello(me - 1)

        for step in (1, 2, -1, -2):
            hello(at_z(step))
        for step in (1, 2, 3):
            hello(at_x(step))

            @pl.when(y + step < YS)
            def _(step=step):
                hello(at_y(step))

    @pl.when(jnp.logical_and(even, jnp.logical_and(z == 0, me > 0)))
    def _():
        hello(me + 3)

    @pl.when(leg_b)
    def _():
        hello(me - 10)

    @pl.when(leg_a)
    def _():
        hello(me + 6)

    pairin[...] = jnp.zeros_like(pairin) + mine

    @pl.when(me == 0)
    def _():
        for g in order:
            near[g][...] = jnp.zeros_like(near[g])

    def end_window(g):
        m = ends[g].shape[0]
        if g == groups:
            for load in series:
                load.wait()
            w = mask[...].astype(jnp.float32)
            v = market[...].astype(jnp.float32) * w
            for t in range(OT):
                tiled[g][RT + t] = jnp.concatenate([v[t : t + 1], w[t : t + 1]], 0).astype(jnp.bfloat16)
        else:
            loads[g].wait()
            for t in range(OT):
                tiled[g][RT + t] = own[g][:, t * LANES : (t + 1) * LANES]
        slot = lambda k: tiled[g][jnp.minimum(jnp.maximum(k, RT), RT + OT - 1)]
        for j, value in enumerate(rolled(slot, mine, RT, m)):
            ends[g][:, j * LANES : (j + 1) * LANES] = value

    def cross(g):
        @pl.when(odd)
        def _():
            remote(ends[g], near[g], near_ssem.at[g], near_rsem.at[g], me - 1).wait_recv()
            short = jnp.maximum(REACH - mine, 0)

            @pl.when(jnp.logical_not(last))
            def _():
                m = ends[g].shape[0]
                for first in range(0, m, 16):
                    part = min(m, 16)
                    b = slice(first, first + part)
                    tail = [near[g][b, QROWS + j * LANES : QROWS + (j + 1) * LANES] for j in range(TT)]
                    placed = moved_right(tail, short, RT + TT)
                    lane = lax.broadcasted_iota(jnp.int32, (part, LANES), 1)
                    for j in range(RT):
                        c = slice(j * LANES, (j + 1) * LANES)
                        send[g][b, c] = jnp.where(lane < short - j * LANES, placed[j + TT], ends[g][b, c])
                if g in around:
                    k = around.index(g)

                    @pl.when(z == ZS - 1)
                    def _():
                        remote(send[g], legs[k], cross_ssem.at[g], leg_rsem.at[k], me - 6).start()

                    @pl.when(z < ZS - 1)
                    def _():
                        remote(send[g], near[g], cross_ssem.at[g], near_rsem.at[g], me + 1).start()
                else:
                    remote(send[g], near[g], cross_ssem.at[g], near_rsem.at[g], me + 1).start()

    def to_partner(g):
        @pl.when(even)
        def _():
            remote(ends[g], near[g], near_ssem.at[g], near_rsem.at[g], me + 1).start()

    for g in order[2:]:
        loads[g].start()
    end_window(order[0])

    @pl.when(odd)
    def _():
        more = jnp.logical_or(jnp.logical_or(leg_a, leg_b), first_leg)
        pl.semaphore_wait(barrier, 2 - jnp.where(last, 1, 0) + jnp.where(more, 1, 0))
        pl.semaphore_signal(present, inc=1, device_id=(me - 1,), device_id_type=MESH)
        remote(pairin, zbuf.at[0], cnt_ssem.at[0], cnt_rsem.at[0], me - 1).start()

    @pl.when(even)
    def _():
        pl.semaphore_wait(present, 1)

    to_partner(order[0])
    end_window(order[1])
    to_partner(order[1])
    cross(order[0])
    cross(order[1])
    for i in range(2, n):
        end_window(order[i])
        to_partner(order[i])
        if i == 2:
            cross(order[i])
        elif i == 3:
            continue
        else:
            cross(order[i - 1])
    cross(order[n - 1])

    def onward_a(k):
        return remote(legs[k], legs[k], leg_ssem.at[k], leg_rsem.at[k], me + 10)

    def onward_b(k):
        return remote(legs[k], near[around[k]], leg_ssem.at[k], near_rsem.at[around[k]], me - 3)

    for on, onward in ((leg_a, onward_a), (leg_b, onward_b)):
        @pl.when(on)
        def _(onward=onward):
            for k in range(len(around)):
                onward_a(k).wait_recv()
                onward(k).start()

    q = lax.broadcasted_iota(jnp.int32, (TILE, TILE), 0)
    p = lax.broadcasted_iota(jnp.int32, (TILE, TILE), 1)
    pre[...] = jnp.where(q <= p, 1.0, 0.0).astype(jnp.bfloat16)
    suf[...] = jnp.where(q > p, 1.0, 0.0).astype(jnp.bfloat16)

    @pl.when(even)
    def _():
        def arrival(dst, k):
            return remote(dst, dst, cnt_ssem.at[k], cnt_rsem.at[k], me + 1)

        sends = []

        def push(ref, target, k):
            copy = remote(ref, ref, cnt_ssem.at[k], cnt_rsem.at[k], target)
            copy.start()
            sends.append(copy)

        pl.semaphore_wait(barrier, 7 + y)
        for step in (1, 2, 3):
            @pl.when(y >= step)
            def _(step=step):
                pl.semaphore_signal(ready, inc=1, device_id=(core0(y - step, x, z),), device_id_type=MESH)

        arrival(zbuf.at[0], 0).wait_recv()
        zbuf[z + 1] = zbuf[0] + mine
        for k, step in ((1, 1), (2, 2), (3, -1), (4, -2)):
            push(zbuf.at[z + 1], at_z(step), k)
        back1, back2 = lax.rem(z + ZS - 1, ZS), lax.rem(z + ZS - 2, ZS)
        ahead1, ahead2 = lax.rem(z + 1, ZS), lax.rem(z + 2, ZS)
        back3, back4, ahead3 = lax.rem(z + ZS - 3, ZS), lax.rem(z + ZS - 4, ZS), lax.rem(z + 3, ZS)
        for k, slot in ((1, back1), (2, back2), (3, ahead1), (4, ahead2)):
            arrival(zbuf.at[slot + 1], k).wait_recv()
        push(zbuf.at[back2 + 1], at_z(1), 5)
        push(zbuf.at[back2 + 1], at_z(2), 6)
        push(zbuf.at[ahead2 + 1], at_z(-1), 7)
        for k, slot in ((5, back3), (6, back4), (7, ahead3)):
            arrival(zbuf.at[slot + 1], k).wait_recv()
        column = zbuf[1]
        below = jnp.where(z > 0, zbuf[1], 0)
        for i in range(1, ZS):
            column = column + zbuf[i + 1]
            below = below + jnp.where(z > i, zbuf[i + 1], 0)
        xbuf[x] = column
        for step in (1, 2, 3):
            push(xbuf.at[x], at_x(step), 7 + step)
        for step in (1, 2, 3):
            arrival(xbuf.at[lax.rem(x + XS - step, XS)], 7 + step).wait_recv()
        plane = xbuf[0]
        below = below + jnp.where(x > 0, xbuf[0], 0)
        for i in range(1, XS):
            plane = plane + xbuf[i]
            below = below + jnp.where(x > i, xbuf[i], 0)
        ybuf[y] = plane
        @pl.when(y < YS - 1)
        def _():
            pl.semaphore_wait(ready, YS - 1 - y)

        for step in (1, 2, 3):
            up = remote(ybuf.at[y], ybuf.at[y], cnt_ssem.at[10 + step], cnt_rsem.at[10 + step], at_y(step))
            pl.when(y + step < YS)(up.start)
        for step in (1, 2, 3):
            @pl.when(y >= step)
            def _(step=step):
                arrival(ybuf.at[y - step], 10 + step).wait_recv()
        for i in range(YS):
            below = below + jnp.where(y > i, ybuf[i], 0)
        ebuf[0] = below - me * QROWS
        ebuf[1] = below + mine - (me + 1) * QROWS
        copy = remote(ebuf.at[pl.ds(0, 2)], ebuf.at[pl.ds(2, 2)], cnt_ssem.at[14], cnt_rsem.at[14], me + 1)
        copy.start()
        sends.append(copy)
        place[0] = ebuf[0]
        place[1] = jnp.full_like(ebuf[0], -1)
        for copy in sends:
            copy.wait_send()
        for step in (1, 2, 3):
            up = remote(ybuf.at[y], ybuf.at[y], cnt_ssem.at[10 + step], cnt_rsem.at[10 + step], at_y(step))
            pl.when(y + step < YS)(up.wait_send)

    @pl.when(odd)
    def _():
        remote(ebuf.at[pl.ds(0, 2)], ebuf.at[pl.ds(2, 2)], cnt_ssem.at[14], cnt_rsem.at[14], me - 1).wait_recv()
        place[0] = ebuf[3]
        place[1] = ebuf[2] - (QROWS - WIN)

    excess = jnp.max(place[0])
    edge = jnp.max(place[1])
    for g in done:
        piece = near[g].at[:, pl.ds(QROWS, WIN)]

        @pl.when(even)
        def _():
            @pl.when(me > 0)
            def _():
                remote(send[g], near[g], cross_ssem.at[g], near_rsem.at[g], me + 1).wait_recv()

            remote(piece, far[g], far_ssem.at[g], far_rsem.at[g], me + 1).start()

        for t in range(RT):
            tiled[g][t] = near[g][:, t * LANES : (t + 1) * LANES]

        @pl.when(odd)
        def _():
            remote(piece, far[g], far_ssem.at[g], far_rsem.at[g], me - 1).wait_recv()
            for t in range(TT):
                fars[g][t] = far[g][:, t * LANES : (t + 1) * LANES]

        ticks = aligned(tiled[g], fars[g], excess, edge)
        if g == groups:
            wx[...] = ticks
            xf = ticks[0:1, :].astype(jnp.float32)
            wf = ticks[1:2, :].astype(jnp.float32)
            row = lax.broadcasted_iota(jnp.int32, (16, REACH), 0)
            a = jnp.where(row == 0, wf, jnp.where(row == 1, xf, xf * xf)).astype(jnp.bfloat16)
            for i, s in enumerate(window_sums(a, pre, suf)):
                c = slice(i * TILE, (i + 1) * TILE)
                sw, sx, sxx = s[0:1], s[1:2], s[2:3]
                stats[0:1, c] = sw
                stats[1:2, c] = sx
                stats[2:3, c] = 1.0 / (sw * sxx - sx * sx + RIDGE * WIN * WIN)
        else:
            m = sizes[g]
            yv = ticks * wx[1:2, :]
            crossed = (wx[0:1, :].astype(jnp.float32) * yv.astype(jnp.float32)).astype(jnp.bfloat16)
            for i, s in enumerate(window_sums(jnp.concatenate([crossed, yv], 0), pre, suf)):
                c = slice(i * TILE, (i + 1) * TILE)
                value = (stats[0:1, c] * s[:m] - stats[1:2, c] * s[m:]) * stats[2:3, c]
                out[starts[g] : starts[g] + m, c] = value

    @pl.when(even)
    def _():
        for g in order:
            remote(ends[g], near[g], near_ssem.at[g], near_rsem.at[g], me + 1).wait_send()
            remote(near[g].at[:, pl.ds(QROWS, WIN)], far[g], far_ssem.at[g], far_rsem.at[g], me + 1).wait_send()

    @pl.when(odd)
    def _():
        remote(pairin, zbuf.at[0], cnt_ssem.at[0], cnt_rsem.at[0], me - 1).wait_send()

        @pl.when(jnp.logical_not(last))
        def _():
            for g in order:
                remote(send[g], near[g], cross_ssem.at[g], near_rsem.at[g], me + 1).wait_send()

        for on, onward in ((leg_a, onward_a), (leg_b, onward_b)):
            @pl.when(on)
            def _(onward=onward):
                for k in range(len(around)):
                    onward(k).wait_send()


def slopes(counts, returns, market, mask, sizes):
    stocks = returns.shape[0]
    bf = jnp.bfloat16

    def per(shape):
        return [pltpu.VMEM(shape(m), bf) for m in list(sizes) + [2]]

    flat = lambda length: per(lambda m: (m, length))
    split = lambda count: per(lambda m: (count, m, LANES))
    n = len(sizes) + 1
    dma = pltpu.SemaphoreType.DMA
    row = lambda k: pltpu.VMEM((k, 1, LANES), jnp.int32)
    vmem = pl.BlockSpec(memory_space=pltpu.VMEM)
    return pl.pallas_call(
        functools.partial(span_kernel, sizes),
        out_shape=jax.ShapeDtypeStruct((stocks, QROWS), jnp.float32),
        in_specs=[pl.BlockSpec(memory_space=pltpu.SMEM)] + [pl.BlockSpec(memory_space=pltpu.HBM)] * 3,
        out_specs=vmem,
        scratch_shapes=flat(REACH) + flat(REACH) + flat(REACH) + flat(WIN) + split(RT + OT) + split(TT)
        + flat(CAP)[:-1]
        + [pltpu.VMEM((1, LANES), jnp.int32), row(ZS + 1), row(XS), row(YS), row(4), row(2)]
        + [pltpu.VMEM((TILE, TILE), bf)] * 2
        + [pltpu.VMEM((8, QROWS), jnp.float32), pltpu.VMEM((2, REACH), bf)]
        + [pltpu.VMEM((OT, LANES), bf), pltpu.VMEM((OT, LANES), jnp.int32)]
        + [dma((n + 1,))] * 6 + [dma((15,))] * 2 + [dma((2,))] * 2 + [pltpu.SemaphoreType.REGULAR] * 2
        + [pltpu.VMEM((sizes[k], REACH), bf) for k in (7, 6)],
        compiler_params=pltpu.CompilerParams(collective_id=0, has_side_effects=True, vmem_limit_bytes=48 << 20),
        name="slopes",
    )(counts, returns, market, mask)


def per_device(returns, market, mask, counts):
    sizes = (16, 16, 32, 32, 32, 32, 32, 32, 16, 16)
    far = lambda a: pltpu.with_memory_space_constraint(a, pltpu.HBM)
    return slopes(counts, returns, far(market.reshape(OT, LANES)), far(mask.reshape(OT, LANES)), sizes)


def solution(mesh):
    return jax.shard_map(
        per_device,
        mesh=mesh,
        in_specs=(P(None, "span"), P("span"), P("span"), P("span")),
        out_specs=P(None, "span"),
        check_vma=False,
    )
```

```python
import functools

import jax
import jax.numpy as jnp
from jax import lax
from jax.experimental import pallas as pl
from jax.experimental.pallas import tpu as pltpu
from jax.sharding import PartitionSpec as P

WIN = 1024
QROWS = 4096
CAP = 2 * QROWS
REACH = QROWS + WIN
RIDGE = 0.1
LANES = 128
TILE = 256
RT = REACH // LANES
OT = CAP // LANES
TT = WIN // LANES
MESH = pl.DeviceIdType.MESH
ZS, XS, YS = 8, 4, 4


def rolled(load, start, tiles, rows):
    first = lax.shift_right_logical(start, 7)
    r = jnp.bitwise_and(start, LANES - 1)
    turn = jnp.bitwise_and(LANES - r, LANES - 1)
    keep = lax.broadcasted_iota(jnp.int32, (rows, LANES), 1) < LANES - r
    turned = [pltpu.roll(load(first + j), turn, 1) for j in range(tiles + 1)]
    return [jnp.where(keep, turned[j], turned[j + 1]) for j in range(tiles)]


def moved_right(tiles, ticks, count):
    r = jnp.bitwise_and(ticks, LANES - 1)
    turned = [pltpu.roll(tile, r, 1) for tile in tiles]
    low = lax.broadcasted_iota(jnp.int32, tiles[0].shape, 1) < r
    n = len(tiles)
    at = {i: jnp.where(low, turned[max(i - 1, 0)], turned[min(i, n - 1)]) for i in range(n + 1)}
    for bit in (32, 16, 8, 4, 2, 1):
        taken = jnp.bitwise_and(ticks, bit * LANES) != 0
        moved = {}
        for i in range(count):
            if i in at and i - bit in at:
                moved[i] = jnp.where(taken, at[i - bit], at[i])
            elif i in at or i - bit in at:
                moved[i] = at[i] if i in at else at[i - bit]
        at = moved
    return at


def aligned(tiles, far_tiles, excess, edge):
    m = tiles.shape[1]
    parts = rolled(lambda k: tiles[jnp.minimum(jnp.maximum(k, 0), RT + OT - 1)], QROWS - excess, RT, m)
    older = rolled(lambda k: far_tiles[jnp.minimum(jnp.maximum(k, 0), TT - 1)], WIN - jnp.maximum(edge, 0), TT, m)
    lane = lax.broadcasted_iota(jnp.int32, (m, LANES), 1)
    for j in range(TT):
        parts[j] = jnp.where(lane < edge - j * LANES, older[j], parts[j])
    return jnp.concatenate(parts, 1)


def window_sums(a, pre, suf):
    m = a.shape[0]
    tiles, halo = REACH // TILE, WIN // TILE
    stack = jnp.concatenate([a[:, t * TILE : (t + 1) * TILE] for t in range(tiles)], 0)
    head = jnp.dot(stack, pre[...], preferred_element_type=jnp.float32)
    tail = jnp.dot(stack[: (tiles - halo) * m], suf[...], preferred_element_type=jnp.float32)
    whole = [head[t * m : (t + 1) * m, TILE - 1 :] for t in range(tiles)]
    result = []
    for t in range(halo, tiles):
        between = whole[t - 3] + whole[t - 2] + whole[t - 1]
        s = t - halo
        result.append(head[t * m : (t + 1) * m] + tail[s * m : (s + 1) * m] + between)
    return result


def span_kernel(sizes, counts, returns, market_in, mask_in, out, *scratch):
    groups = len(sizes)
    starts = [sum(sizes[:g]) for g in range(groups)]
    n = groups + 1
    it = iter(scratch)
    take = lambda k=n: [next(it) for _ in range(k)]
    ends, send, near, far, tiled, fars = take(), take(), take(), take(), take(), take()
    own = take(groups)
    pairin, zbuf, xbuf, ybuf, ebuf, place = take(6)
    pre, suf, stats, wx, market, mask = take(6)
    own_sem, near_ssem, cross_ssem, near_rsem, far_ssem, far_rsem, cnt_ssem, cnt_rsem, leg_ssem, leg_rsem, present, ready = take(12)
    step_ssem, step_rsem, okay = take(3)
    legs = take(2)
    stepped = next(it)

    me = lax.axis_index("span")
    total = ZS * XS * YS * 2
    even = lax.rem(me, 2) == 0
    odd = lax.rem(me, 2) == 1
    last = me == total - 1
    chip = lax.div(me, 2)
    z = lax.rem(chip, ZS)
    x = lax.rem(lax.div(chip, ZS), XS)
    y = lax.div(chip, ZS * XS)

    odd_core = lax.rem(me, 2) == 1

    def core0(yy, xx, zz):
        return ((yy * XS + xx) * ZS + zz) * 2

    def at_z(step):
        return core0(y, x, lax.rem(z + step + ZS, ZS))

    def at_x(step):
        return core0(y, lax.rem(x + step, XS), z)

    def at_y(step):
        return core0(lax.rem(y + step, YS), x, z)

    around = [7, 6]
    rest = [k for k in range(1, groups) if k not in around]
    order = [0, groups] + around + rest
    done = [groups, 0] + rest[1:-2] + around + [1] + rest[-2:]
    column = lax.div(me, 2 * ZS)
    inner = column < XS * YS - 1
    leg_a = jnp.logical_and(odd_core, jnp.logical_and(inner, z == 4))
    leg_b = jnp.logical_and(odd_core, jnp.logical_and(column > 0, z == 1))
    step_a = jnp.logical_and(odd_core, z == 0)
    step_b = jnp.logical_and(odd_core, z == 5)
    first_leg = jnp.logical_and(odd_core, jnp.logical_and(inner, z == 7))

    def remote(src, dst, ssem, rsem, target):
        return pltpu.make_async_remote_copy(
            src_ref=src, dst_ref=dst, send_sem=ssem, recv_sem=rsem, device_id=(target,), device_id_type=MESH
        )

    series = [
        pltpu.make_async_copy(market_in, market, own_sem.at[groups]),
        pltpu.make_async_copy(mask_in, mask, own_sem.at[n]),
    ]
    loads = [
        pltpu.make_async_copy(returns.at[pl.ds(starts[g], sizes[g]), :], own[g], own_sem.at[g]) for g in range(groups)
    ]
    loads[0].start()
    for load in series:
        load.start()

    barrier = pltpu.get_barrier_semaphore()

    def hello(target):
        pl.semaphore_signal(barrier, inc=1, device_id=(target,), device_id_type=MESH)

    mine = counts[0]

    @pl.when(even)
    def _():
        hello(me + 1)

        @pl.when(me > 0)
        def _():
            hello(me - 1)

        for step in (1, 2, -1, -2):
            hello(at_z(step))
        for step in (1, 2, 3):
            hello(at_x(step))

            @pl.when(y + step < YS)
            def _(step=step):
                hello(at_y(step))

    @pl.when(jnp.logical_and(even, jnp.logical_and(z == 0, me > 0)))
    def _():
        hello(me + 3)

    @pl.when(jnp.logical_and(even, z == 4))
    def _():
        hello(me + 3)

    @pl.when(step_a)
    def _():
        hello(me + 6)
        hello(me + 10)

    @pl.when(leg_b)
    def _():
        hello(me - 10)

    @pl.when(leg_a)
    def _():
        hello(me + 6)

    pairin[...] = jnp.zeros_like(pairin) + mine

    @pl.when(me == 0)
    def _():
        for g in order:
            near[g][...] = jnp.zeros_like(near[g])

    def end_window(g):
        m = ends[g].shape[0]
        if g == groups:
            for load in series:
                load.wait()
            w = mask[...].astype(jnp.float32)
            v = market[...].astype(jnp.float32) * w
            for t in range(OT):
                tiled[g][RT + t] = jnp.concatenate([v[t : t + 1], w[t : t + 1]], 0).astype(jnp.bfloat16)
        else:
            loads[g].wait()
            for t in range(OT):
                tiled[g][RT + t] = own[g][:, t * LANES : (t + 1) * LANES]
        slot = lambda k: tiled[g][jnp.minimum(jnp.maximum(k, RT), RT + OT - 1)]
        for j, value in enumerate(rolled(slot, mine, RT, m)):
            ends[g][:, j * LANES : (j + 1) * LANES] = value

    def cross(g):
        @pl.when(odd)
        def _():
            remote(ends[g], near[g], near_ssem.at[g], near_rsem.at[g], me - 1).wait_recv()
            short = jnp.maximum(REACH - mine, 0)

            @pl.when(jnp.logical_not(last))
            def _():
                m = ends[g].shape[0]
                for first in range(0, m, 16):
                    part = min(m, 16)
                    b = slice(first, first + part)
                    tail = [near[g][b, QROWS + j * LANES : QROWS + (j + 1) * LANES] for j in range(TT)]
                    placed = moved_right(tail, short, RT + TT)
                    lane = lax.broadcasted_iota(jnp.int32, (part, LANES), 1)
                    for j in range(RT):
                        c = slice(j * LANES, (j + 1) * LANES)
                        send[g][b, c] = jnp.where(lane < short - j * LANES, placed[j + TT], ends[g][b, c])
                if g in around:
                    k = around.index(g)

                    @pl.when(z == ZS - 1)
                    def _():
                        remote(send[g], legs[k], cross_ssem.at[g], leg_rsem.at[k], me - 6).start()

                    @pl.when(z < ZS - 1)
                    def _():
                        remote(send[g], near[g], cross_ssem.at[g], near_rsem.at[g], me + 1).start()
                elif g == 1:
                    @pl.when(z == 3)
                    def _():
                        remote(send[g], stepped, cross_ssem.at[g], step_rsem, me - 6).start()

                    @pl.when(z != 3)
                    def _():
                        remote(send[g], near[g], cross_ssem.at[g], near_rsem.at[g], me + 1).start()
                else:
                    remote(send[g], near[g], cross_ssem.at[g], near_rsem.at[g], me + 1).start()

    def to_partner(g):
        @pl.when(even)
        def _():
            remote(ends[g], near[g], near_ssem.at[g], near_rsem.at[g], me + 1).start()

    for g in order[2:]:
        loads[g].start()
    end_window(order[0])

    @pl.when(odd)
    def _():
        more = jnp.logical_or(jnp.logical_or(leg_a, leg_b), jnp.logical_or(first_leg, z == 3))
        pl.semaphore_wait(barrier, 2 - jnp.where(last, 1, 0) + jnp.where(more, 1, 0) + jnp.where(z == 5, 2, 0))
        @pl.when(z == 5)
        def _():
            pl.semaphore_signal(okay, inc=1, device_id=(me - 10,), device_id_type=MESH)

        pl.semaphore_signal(present, inc=1, device_id=(me - 1,), device_id_type=MESH)
        remote(pairin, zbuf.at[0], cnt_ssem.at[0], cnt_rsem.at[0], me - 1).start()

    @pl.when(even)
    def _():
        pl.semaphore_wait(present, 1)

    to_partner(order[0])
    end_window(order[1])
    to_partner(order[1])
    cross(order[0])
    cross(order[1])
    for i in range(2, n):
        end_window(order[i])
        to_partner(order[i])
        if i == 2:
            cross(order[i])
        elif i == 3:
            continue
        else:
            cross(order[i - 1])
    cross(order[n - 1])

    def onward_a(k):
        return remote(legs[k], legs[k], leg_ssem.at[k], leg_rsem.at[k], me + 10)

    def onward_b(k):
        return remote(legs[k], near[around[k]], leg_ssem.at[k], near_rsem.at[around[k]], me - 3)

    onto_b = remote(stepped, stepped, step_ssem, step_rsem, me + 10)
    onto_c = remote(stepped, near[1], step_ssem, near_rsem.at[1], me - 3)

    @pl.when(step_a)
    def _():
        onto_b.wait_recv()
        pl.semaphore_wait(okay, 1)
        onto_b.start()

    @pl.when(step_b)
    def _():
        onto_b.wait_recv()
        onto_c.start()

    for on, onward in ((leg_a, onward_a), (leg_b, onward_b)):
        @pl.when(on)
        def _(onward=onward):
            for k in range(len(around)):
                onward_a(k).wait_recv()
                onward(k).start()

    q = lax.broadcasted_iota(jnp.int32, (TILE, TILE), 0)
    p = lax.broadcasted_iota(jnp.int32, (TILE, TILE), 1)
    pre[...] = jnp.where(q <= p, 1.0, 0.0).astype(jnp.bfloat16)
    suf[...] = jnp.where(q > p, 1.0, 0.0).astype(jnp.bfloat16)

    @pl.when(even)
    def _():
        def arrival(dst, k):
            return remote(dst, dst, cnt_ssem.at[k], cnt_rsem.at[k], me + 1)

        sends = []

        def push(ref, target, k):
            copy = remote(ref, ref, cnt_ssem.at[k], cnt_rsem.at[k], target)
            copy.start()
            sends.append(copy)

        pl.semaphore_wait(barrier, 7 + y)
        for step in (1, 2, 3):
            @pl.when(y >= step)
            def _(step=step):
                pl.semaphore_signal(ready, inc=1, device_id=(core0(y - step, x, z),), device_id_type=MESH)

        arrival(zbuf.at[0], 0).wait_recv()
        zbuf[z + 1] = zbuf[0] + mine
        for k, step in ((1, 1), (2, 2), (3, -1), (4, -2)):
            push(zbuf.at[z + 1], at_z(step), k)
        back1, back2 = lax.rem(z + ZS - 1, ZS), lax.rem(z + ZS - 2, ZS)
        ahead1, ahead2 = lax.rem(z + 1, ZS), lax.rem(z + 2, ZS)
        back3, back4, ahead3 = lax.rem(z + ZS - 3, ZS), lax.rem(z + ZS - 4, ZS), lax.rem(z + 3, ZS)
        for k, slot in ((1, back1), (2, back2), (3, ahead1), (4, ahead2)):
            arrival(zbuf.at[slot + 1], k).wait_recv()
        push(zbuf.at[back2 + 1], at_z(1), 5)
        push(zbuf.at[back2 + 1], at_z(2), 6)
        push(zbuf.at[ahead2 + 1], at_z(-1), 7)
        for k, slot in ((5, back3), (6, back4), (7, ahead3)):
            arrival(zbuf.at[slot + 1], k).wait_recv()
        column = zbuf[1]
        below = jnp.where(z > 0, zbuf[1], 0)
        for i in range(1, ZS):
            column = column + zbuf[i + 1]
            below = below + jnp.where(z > i, zbuf[i + 1], 0)
        xbuf[x] = column
        for step in (1, 2, 3):
            push(xbuf.at[x], at_x(step), 7 + step)
        for step in (1, 2, 3):
            arrival(xbuf.at[lax.rem(x + XS - step, XS)], 7 + step).wait_recv()
        plane = xbuf[0]
        below = below + jnp.where(x > 0, xbuf[0], 0)
        for i in range(1, XS):
            plane = plane + xbuf[i]
            below = below + jnp.where(x > i, xbuf[i], 0)
        ybuf[y] = plane
        @pl.when(y < YS - 1)
        def _():
            pl.semaphore_wait(ready, YS - 1 - y)

        for step in (1, 2, 3):
            up = remote(ybuf.at[y], ybuf.at[y], cnt_ssem.at[10 + step], cnt_rsem.at[10 + step], at_y(step))
            pl.when(y + step < YS)(up.start)
        for step in (1, 2, 3):
            @pl.when(y >= step)
            def _(step=step):
                arrival(ybuf.at[y - step], 10 + step).wait_recv()
        for i in range(YS):
            below = below + jnp.where(y > i, ybuf[i], 0)
        ebuf[0] = below - me * QROWS
        ebuf[1] = below + mine - (me + 1) * QROWS
        copy = remote(ebuf.at[pl.ds(0, 2)], ebuf.at[pl.ds(2, 2)], cnt_ssem.at[14], cnt_rsem.at[14], me + 1)
        copy.start()
        sends.append(copy)
        place[0] = ebuf[0]
        place[1] = jnp.full_like(ebuf[0], -1)
        for copy in sends:
            copy.wait_send()
        for step in (1, 2, 3):
            up = remote(ybuf.at[y], ybuf.at[y], cnt_ssem.at[10 + step], cnt_rsem.at[10 + step], at_y(step))
            pl.when(y + step < YS)(up.wait_send)

    @pl.when(odd)
    def _():
        remote(ebuf.at[pl.ds(0, 2)], ebuf.at[pl.ds(2, 2)], cnt_ssem.at[14], cnt_rsem.at[14], me - 1).wait_recv()
        place[0] = ebuf[3]
        place[1] = ebuf[2] - (QROWS - WIN)

    excess = jnp.max(place[0])
    edge = jnp.max(place[1])
    for g in done:
        piece = near[g].at[:, pl.ds(QROWS, WIN)]

        @pl.when(even)
        def _():
            @pl.when(me > 0)
            def _():
                remote(send[g], near[g], cross_ssem.at[g], near_rsem.at[g], me + 1).wait_recv()

            remote(piece, far[g], far_ssem.at[g], far_rsem.at[g], me + 1).start()

        for t in range(RT):
            tiled[g][t] = near[g][:, t * LANES : (t + 1) * LANES]

        @pl.when(odd)
        def _():
            remote(piece, far[g], far_ssem.at[g], far_rsem.at[g], me - 1).wait_recv()
            for t in range(TT):
                fars[g][t] = far[g][:, t * LANES : (t + 1) * LANES]

        ticks = aligned(tiled[g], fars[g], excess, edge)
        if g == groups:
            wx[...] = ticks
            xf = ticks[0:1, :].astype(jnp.float32)
            wf = ticks[1:2, :].astype(jnp.float32)
            row = lax.broadcasted_iota(jnp.int32, (16, REACH), 0)
            a = jnp.where(row == 0, wf, jnp.where(row == 1, xf, xf * xf)).astype(jnp.bfloat16)
            for i, s in enumerate(window_sums(a, pre, suf)):
                c = slice(i * TILE, (i + 1) * TILE)
                sw, sx, sxx = s[0:1], s[1:2], s[2:3]
                stats[0:1, c] = sw
                stats[1:2, c] = sx
                stats[2:3, c] = 1.0 / (sw * sxx - sx * sx + RIDGE * WIN * WIN)
        else:
            m = sizes[g]
            yv = ticks * wx[1:2, :]
            crossed = (wx[0:1, :].astype(jnp.float32) * yv.astype(jnp.float32)).astype(jnp.bfloat16)
            for i, s in enumerate(window_sums(jnp.concatenate([crossed, yv], 0), pre, suf)):
                c = slice(i * TILE, (i + 1) * TILE)
                value = (stats[0:1, c] * s[:m] - stats[1:2, c] * s[m:]) * stats[2:3, c]
                out[starts[g] : starts[g] + m, c] = value

    @pl.when(even)
    def _():
        for g in order:
            remote(ends[g], near[g], near_ssem.at[g], near_rsem.at[g], me + 1).wait_send()
            remote(near[g].at[:, pl.ds(QROWS, WIN)], far[g], far_ssem.at[g], far_rsem.at[g], me + 1).wait_send()

    @pl.when(odd)
    def _():
        remote(pairin, zbuf.at[0], cnt_ssem.at[0], cnt_rsem.at[0], me - 1).wait_send()

        @pl.when(jnp.logical_not(last))
        def _():
            for g in order:
                remote(send[g], near[g], cross_ssem.at[g], near_rsem.at[g], me + 1).wait_send()

        for on, onward in ((leg_a, onward_a), (leg_b, onward_b)):
            @pl.when(on)
            def _(onward=onward):
                for k in range(len(around)):
                    onward(k).wait_send()

        pl.when(step_a)(onto_b.wait_send)
        pl.when(step_b)(onto_c.wait_send)


def slopes(counts, returns, market, mask, sizes):
    stocks = returns.shape[0]
    bf = jnp.bfloat16

    def per(shape):
        return [pltpu.VMEM(shape(m), bf) for m in list(sizes) + [2]]

    flat = lambda length: per(lambda m: (m, length))
    split = lambda count: per(lambda m: (count, m, LANES))
    n = len(sizes) + 1
    dma = pltpu.SemaphoreType.DMA
    row = lambda k: pltpu.VMEM((k, 1, LANES), jnp.int32)
    vmem = pl.BlockSpec(memory_space=pltpu.VMEM)
    return pl.pallas_call(
        functools.partial(span_kernel, sizes),
        out_shape=jax.ShapeDtypeStruct((stocks, QROWS), jnp.float32),
        in_specs=[pl.BlockSpec(memory_space=pltpu.SMEM)] + [pl.BlockSpec(memory_space=pltpu.HBM)] * 3,
        out_specs=vmem,
        scratch_shapes=flat(REACH) + flat(REACH) + flat(REACH) + flat(WIN) + split(RT + OT) + split(TT)
        + flat(CAP)[:-1]
        + [pltpu.VMEM((1, LANES), jnp.int32), row(ZS + 1), row(XS), row(YS), row(4), row(2)]
        + [pltpu.VMEM((TILE, TILE), bf)] * 2
        + [pltpu.VMEM((8, QROWS), jnp.float32), pltpu.VMEM((2, REACH), bf)]
        + [pltpu.VMEM((OT, LANES), bf), pltpu.VMEM((OT, LANES), jnp.int32)]
        + [dma((n + 1,))] * 6 + [dma((15,))] * 2 + [dma((2,))] * 2 + [pltpu.SemaphoreType.REGULAR] * 2 + [dma] * 2 + [pltpu.SemaphoreType.REGULAR]
        + [pltpu.VMEM((sizes[k], REACH), bf) for k in (7, 6)] + [pltpu.VMEM((sizes[1], REACH), bf)],
        compiler_params=pltpu.CompilerParams(collective_id=0, has_side_effects=True, vmem_limit_bytes=48 << 20),
        name="slopes",
    )(counts, returns, market, mask)


def per_device(returns, market, mask, counts):
    sizes = (16, 16, 32, 32, 32, 32, 32, 32, 16, 16)
    far = lambda a: pltpu.with_memory_space_constraint(a, pltpu.HBM)
    return slopes(counts, returns, far(market.reshape(OT, LANES)), far(mask.reshape(OT, LANES)), sizes)


def solution(mesh):
    return jax.shard_map(
        per_device,
        mesh=mesh,
        in_specs=(P(None, "span"), P("span"), P("span"), P("span")),
        out_specs=P(None, "span"),
        check_vma=False,
    )
```
